256 devices in a mesh: mkt: 32 (over z, y), draw: 8 (over x, core).
Axes of the slice: x: 4, y: 4, z: 8, core: 2. Of those that a mesh axis runs over, the one named last changes fastest.
Arguments:
- x_char: float32 [1536, 56, 8], P('mkt'), may hold values from -2.5 to 2.5
- nu_draws: float32 [1536, 8, 4096], P('mkt', None, 'draw'), may hold values from -3 to 3
- coef_sigma: float32 [8], replicated, may hold values from 0.3 to 1.2
- log_share: float32 [1536, 56], P('mkt'), may hold values from -7 to -4.5
- counts: int32 [1536], P('mkt'), may hold values from 28 to 56
Outputs:
- mean_util: float32 [1536, 56], P('mkt')
- jacobian: float32 [1536, 56, 56], P(('mkt', 'draw'))
- sup_norms: float32 [3], replicated
The draws below stay inside these ranges and needn't reach their ends.
Inputs may be any that keep to these rules, and one draw needn't show every extreme that they name: Products 0 to counts - 1 of a market are valid; the other slots are padding.
All inputs are finite; a program needn't handle non-finite values. Where the reference program divides by a largest or mean magnitude, that divisor is 1e-20 or more.
Results may differ from the reference program's by a relative error of at most 0.00013.
Values sent between devices are 32-bit elements; how exact they have to be, the bound alone decides.
No kernel may reach another device: no remote copies, remote signals or barrier semaphores. Data moves between devices by JAX's collectives and lax.ppermute only.
A program may use at most 64 MiB of HBM per device.

```python
import math
import jax
import jax.numpy as jnp
from jax import lax

J = 56
K = 8
ITERS = 3
M = 1536
R = 4096


def set_ends(array, key, least, top_value):
    longest = array.shape.index(max(array.shape))
    spots = []
    for shift in (0, 1):
        where = [jax.random.randint(jax.random.fold_in(key, axis), (), 0, length) for axis, length in enumerate(array.shape)]
        where[longest] = (where[longest] + shift) % array.shape[longest]
        spots.append(tuple(where))
    return array.at[spots[0]].set(least).at[spots[1]].set(top_value)


def shard_levels(key, shape, pieces, least, top_value):
    gain, own = 1.0, jax.random.fold_in(key, 6)
    for position, blocks in pieces:
        heights = jnp.exp(jax.random.uniform(jax.random.fold_in(own, position), (blocks,), jnp.float32, least / len(pieces), top_value / len(pieces)))
        gain = gain * jnp.repeat(heights, shape[position] // blocks).reshape([-1 if axis == position else 1 for axis in range(len(shape))])
    return gain


def gaussian(key, shape, spread, bound, cuts=(), kind=jnp.bfloat16):
    array = spread * jax.random.normal(key, shape, jnp.float32)
    if cuts:
        array = array * shard_levels(key, shape, cuts, -0.22, 0.18)
    return jnp.clip(array, -bound, bound).astype(kind)


def setup_inputs(seed: int = 0) -> dict:
    seeds = jax.random.split(jax.random.key(seed), 6)
    return {
        "x_char": gaussian(seeds[0], (M, J, K), 1.0, 2.5, ((0, 32),), jnp.float32),
        "nu_draws": gaussian(seeds[1], (M, K, R), 1.0, 3.0, ((0, 32), (2, 8)), jnp.float32),
        "coef_sigma": jnp.clip(jnp.exp(jax.random.uniform(seeds[2], (K,), jnp.float32, math.log(0.3), math.log(1.2))), 0.3, 1.2),
        "log_share": jnp.clip(-7.0 + 2.5 * jax.random.uniform(seeds[3], (M, J), jnp.float32) ** shard_levels(seeds[3], (M, J), ((0, 32),), -0.2, 0.2), -7.0, -4.5),
        "counts": set_ends(jax.random.randint(seeds[4], (M,), J // 2, J + 1), jax.random.fold_in(seeds[4], 1), J // 2, J).astype(jnp.int32),
    }


step_cap = 0.25
epsilon = 1e-6


def market_terms(mean_util, scaled, nu_draws, usable, inverse, with_products):
    tastes = jnp.einsum("mjk,mkr->mjr", scaled, nu_draws, precision=lax.Precision.HIGHEST)
    raised = jnp.where(usable[:, :, None], jnp.exp(mean_util[:, :, None] + tastes), 0.0)
    chance = raised / (1.0 + jnp.sum(raised, axis=1, keepdims=True))
    shares = jnp.sum(chance, axis=2) * inverse
    if with_products:
        cross_sums = jnp.einsum("mjr,mlr->mjl", chance, chance, precision=lax.Precision.HIGHEST) * inverse
        return shares, cross_sums
    return shares


def evaluate(mean_util, scaled, nu_draws, usable, inverse, with_products):
    groups = mean_util.shape[0] // 8
    folded = (mean_util.reshape(groups, 8, mean_util.shape[1]),
              scaled.reshape(groups, 8, scaled.shape[1], scaled.shape[2]),
              nu_draws.reshape(groups, 8, nu_draws.shape[1], nu_draws.shape[2]),
              usable.reshape(groups, 8, usable.shape[1]))

    def per_group(items):
        return market_terms(items[0], items[1], items[2], items[3], inverse, with_products)

    def unfold(member):
        return member.reshape((groups * 8,) + member.shape[2:])

    return jax.tree.map(unfold, lax.map(per_group, folded))


def reference(x_char, nu_draws, coef_sigma, log_share, counts):
    usable = jnp.arange(J, dtype=jnp.int32)[None, :] < counts[:, None]
    scaled = x_char * coef_sigma[None, None, :]
    inverse = 1.0 / R
    inside = jnp.sum(jnp.where(usable, jnp.exp(log_share), 0.0), axis=1)
    mean_util = jnp.where(usable, log_share - jnp.log(1.0 - inside)[:, None], 0.0)
    norms_list = []
    for sweep in range(ITERS):
        shares = evaluate(mean_util, scaled, nu_draws, usable, inverse, False)
        change = jnp.where(usable, log_share - jnp.log(jnp.where(usable, shares, 1.0)), 0.0)
        largest = jnp.max(jnp.abs(change))
        mean_util = mean_util + jnp.minimum(1.0, step_cap / (largest + epsilon)) * change
        norms_list.append(largest)
    shares, cross_sums = evaluate(mean_util, scaled, nu_draws, usable, inverse, True)
    divisor = jnp.where(usable, shares, 1.0)
    identity = jnp.eye(J, dtype=jnp.float32)
    paired = usable[:, :, None] & usable[:, None, :]
    jacobian = jnp.where(paired, identity[None, :, :] - cross_sums / divisor[:, :, None], 0.0)
    return mean_util, jacobian, jnp.stack(norms_list)
```

```python
import jax
import jax.numpy as jnp
from jax import lax
from jax.experimental import pallas as pl
from jax.experimental.pallas import tpu as pltpu
from jax.sharding import PartitionSpec as P

step_cap = 0.25
epsilon = 1e-06
LOG2E = 1.4426950408889634
VMEM = pl.BlockSpec(memory_space=pltpu.VMEM)
SMEM = pl.BlockSpec(memory_space=pltpu.SMEM)
EVERY = ("mkt", "draw")


def pieces(value):
    high = value.astype(jnp.bfloat16).astype(jnp.float32)
    rest = value - high
    middle = rest.astype(jnp.bfloat16).astype(jnp.float32)
    return high, middle, rest - middle


def first_market(own):
    return lax.axis_index("draw") * own


def fill(ref, value):
    tile = jnp.broadcast_to(value, (8, ref.shape[1]))
    for row in range(0, ref.shape[0], 8):
        ref[row : row + 8, :] = tile


def column(value, slot, lanes=128):
    return jnp.broadcast_to(value[:, slot : slot + 1], (value.shape[0], lanes))


def share_columns(weights, raised_ref, own):
    slots, width = weights.shape
    draws = raised_ref.shape[2]
    lane = lax.broadcasted_iota(jnp.int32, (slots, width), 1)
    totals = jnp.ones((slots, width), jnp.float32)
    for m in range(own):
        weight = column(weights, m)
        total = jnp.zeros((slots, 128), jnp.float32)
        for g in range(0, draws, 128):
            raised = raised_ref[m, :, g : g + 128]
            below = 1.0 + jnp.sum(raised * weight, axis=0, keepdims=True)
            total = total + raised * (1.0 / below)
        totals = jnp.where(lane == m, jnp.sum(total, axis=1, keepdims=True), totals)
    return totals * weights * (1.0 / draws)


def contraction(state_ref, mean_util, raised_ref, own):
    log_share, usable = state_ref[0], state_ref[1] > 0.0
    weights = jnp.where(usable, jnp.exp(mean_util), 0.0)
    shares = share_columns(weights, raised_ref, own)
    return jnp.where(usable, log_share - jnp.log(jnp.where(usable, shares, 1.0)), 0.0)


def start_kernel(own, counts_ref, sigma_ref, log_share_ref, x_ref, nu_ref, raised_ref, state_ref, peak_ref, rows_ref):
    base = first_market(own)
    slots = log_share_ref.shape[1]
    depth = x_ref.shape[1]
    span = nu_ref.shape[2]
    level = lax.broadcasted_iota(jnp.int32, (depth, slots), 0)
    sigma = jnp.zeros((depth, slots), jnp.float32)
    for k in range(depth):
        sigma = jnp.where(level == k, sigma_ref[k], sigma)
    for m in range(own):
        high, middle, low = pieces(x_ref[base + m] * sigma * LOG2E)
        left = jnp.concatenate([high, high, middle, high, low, middle], axis=0)
        left = jnp.transpose(left).astype(jnp.bfloat16)
        for s in range(nu_ref.shape[0] // own):
            high, middle, low = pieces(nu_ref[s * own + m])
            right = jnp.concatenate([high, middle, high, low, high, middle], axis=0)
            tastes = jnp.dot(left, right.astype(jnp.bfloat16), preferred_element_type=jnp.float32)
            raised_ref[m, :, s * span : (s + 1) * span] = jnp.exp2(tastes)
    rows_ref[...] = jnp.zeros_like(rows_ref)
    for m in range(own):
        rows_ref[m : m + 1, 0:slots] = log_share_ref[pl.ds(base + m, 1), :]
    log_share = jnp.transpose(rows_ref[...])[0:slots, :]
    slot = lax.broadcasted_iota(jnp.int32, (slots, 8), 0)
    lane = lax.broadcasted_iota(jnp.int32, (slots, 8), 1)
    count = jnp.zeros((slots, 8), jnp.int32)
    for m in range(own):
        count = jnp.where(lane == m, counts_ref[base + m], count)
    usable = slot < count
    inside = jnp.sum(jnp.where(usable, jnp.exp(log_share), 0.0), axis=0, keepdims=True)
    mean_util = jnp.where(usable, log_share - jnp.log(1.0 - inside), 0.0)
    state_ref[0] = log_share
    state_ref[1] = jnp.where(usable, 1.0, 0.0)
    state_ref[2] = mean_util
    change = contraction(state_ref, mean_util, raised_ref, own)
    state_ref[3] = change
    state_ref[4] = jnp.zeros_like(change)
    fill(peak_ref, jnp.max(jnp.abs(change)))


def moved(peaks_ref, state_ref):
    largest = jnp.max(peaks_ref[...])
    step = jnp.minimum(1.0, step_cap / (largest + epsilon))
    return largest, state_ref[2] + step * state_ref[3]


def norm_row(turn, largest, state_ref):
    row = lax.broadcasted_iota(jnp.int32, state_ref.shape[1:], 0)
    return jnp.where(row == turn, largest, state_ref[4])


def next_kernel(own, turn, peaks_ref, state_ref, raised_ref, out_ref, peak_ref):
    largest, mean_util = moved(peaks_ref, state_ref)
    change = contraction(state_ref, mean_util, raised_ref, own)
    out_ref[0] = state_ref[0]
    out_ref[1] = state_ref[1]
    out_ref[2] = mean_util
    out_ref[3] = change
    out_ref[4] = norm_row(turn, largest, state_ref)
    fill(peak_ref, jnp.max(jnp.abs(change)))


def settle_kernel(own, turn, peaks_ref, state_ref, out_ref, copies_ref, norms_ref):
    largest, mean_util = moved(peaks_ref, state_ref)
    out_ref[...] = mean_util
    norms = norm_row(turn, largest, state_ref)
    for t in range(turn + 1):
        norms_ref[t] = jnp.max(norms[t : t + 1, :])
    slots = mean_util.shape[0]
    padded = jnp.concatenate([mean_util, jnp.zeros((128 - slots, 8), jnp.float32)], axis=0)
    rows = jnp.transpose(padded)
    for d in range(copies_ref.shape[0]):
        copies_ref[d] = rows


def final_kernel(own, counts_ref, mean_ref, raised_ref, jacobian_ref, high_ref, both_ref):
    base = first_market(own)
    mean_util = mean_ref[...]
    slots = mean_util.shape[0]
    draws = raised_ref.shape[2]
    padding = jnp.zeros((64 - slots, 128), jnp.float32)
    row = lax.broadcasted_iota(jnp.int32, (slots, slots), 0)
    col = lax.broadcasted_iota(jnp.int32, (slots, slots), 1)
    slot = lax.broadcasted_iota(jnp.int32, (slots, 128), 0)
    for m in range(own):
        count = counts_ref[base + m]
        weight = jnp.where(slot < count, jnp.exp(column(mean_util, m)), 0.0)
        total = jnp.zeros((slots, 128), jnp.float32)
        buffer = m % 2
        for g in range(0, draws, 128):
            raised = raised_ref[m, :, g : g + 128] * weight
            chance = raised * (1.0 / (1.0 + jnp.sum(raised, axis=0, keepdims=True)))
            total = total + chance
            padded = jnp.concatenate([chance, padding], axis=0)
            high = padded.astype(jnp.bfloat16)
            low = (padded - high.astype(jnp.float32)).astype(jnp.bfloat16)
            both_ref[buffer, 0:64, g : g + 128] = high
            both_ref[buffer, 64:128, g : g + 128] = low
        product = lax.dot_general(
            both_ref[buffer, 0:64, :],
            both_ref[buffer],
            (((1,), (1,)), ((), ())),
            preferred_element_type=jnp.float32,
        )
        crossed = product[:, 64:128]
        cross = (product[:, 0:64] + crossed + jnp.transpose(crossed))[0:slots, 0:slots]
        shares = jnp.sum(total, axis=1, keepdims=True)
        divisor = jnp.where(row < count, shares, 1.0)
        identity = jnp.where(row == col, 1.0, 0.0)
        jacobian_ref[m] = jnp.where((row < count) & (col < count), identity - cross / divisor, 0.0)


def params(mebibytes=16):
    return pltpu.CompilerParams(vmem_limit_bytes=mebibytes << 20)


def shards(x_char, nu_draws, coef_sigma, log_share, counts):
    markets, slots = log_share.shape
    depth, span = nu_draws.shape[1:]
    draw_count, every = lax.axis_size("draw"), lax.axis_size(EVERY)
    own = markets // draw_count
    f32 = jnp.float32
    raised_shape = jax.ShapeDtypeStruct((own, slots, span * draw_count), f32)
    state_shape = jax.ShapeDtypeStruct((5, slots, 8), f32)
    peak_shape = jax.ShapeDtypeStruct((every, 128), f32)

    def everywhere(peak):
        return lax.all_to_all(peak.reshape(every, 1, 128), EVERY, 0, 0, tiled=True).reshape(every, 128)

    nu_own = lax.all_to_all(nu_draws, "draw", 0, 0, tiled=True)
    raised, state, peak = pl.pallas_call(
        lambda *refs: start_kernel(own, *refs),
        out_shape=(raised_shape, state_shape, peak_shape),
        in_specs=[SMEM, SMEM, VMEM, VMEM, VMEM],
        out_specs=(VMEM, VMEM, VMEM),
        scratch_shapes=[pltpu.VMEM((8, 128), f32)],
        compiler_params=params(),
        name="start",
    )(counts, coef_sigma, log_share, jnp.transpose(x_char, (0, 2, 1)), nu_own)
    for turn in range(2):
        state, peak = pl.pallas_call(
            lambda *refs, turn=turn: next_kernel(own, turn, *refs),
            out_shape=(state_shape, peak_shape),
            in_specs=[VMEM, VMEM, VMEM],
            out_specs=(VMEM, VMEM),
            compiler_params=params(),
            name="next",
        )(everywhere(peak), state, raised)
    mean_own, copies, norms = pl.pallas_call(
        lambda *refs: settle_kernel(own, 2, *refs),
        out_shape=(
            jax.ShapeDtypeStruct((slots, 8), f32),
            jax.ShapeDtypeStruct((draw_count, 8, 128), f32),
            jax.ShapeDtypeStruct((3,), f32),
        ),
        in_specs=[VMEM, VMEM],
        out_specs=(VMEM, VMEM, SMEM),
        compiler_params=params(),
        name="settle",
    )(everywhere(peak), state)
    gathered = lax.all_to_all(copies, "draw", 0, 0, tiled=True)
    jacobian = pl.pallas_call(
        lambda *refs: final_kernel(own, *refs),
        out_shape=jax.ShapeDtypeStruct((own, slots, slots), f32),
        in_specs=[SMEM, VMEM, VMEM],
        out_specs=VMEM,
        scratch_shapes=[pltpu.VMEM((8, 128), f32), pltpu.VMEM((2, 128, span * draw_count), jnp.bfloat16)],
        compiler_params=params(),
        cost_estimate=pl.CostEstimate(flops=2_000_000_000, bytes_accessed=8_000_000, transcendentals=0),
        name="final",
    )(counts, mean_own, raised)
    mean_util = gathered[:, :own, :slots].reshape(markets, slots)
    return (mean_util, jacobian, norms)


def solution(mesh):
    return jax.shard_map(
        shards,
        mesh=mesh,
        in_specs=(P("mkt", None, None), P("mkt", None, "draw"), P(), P("mkt", None), P("mkt")),
        out_specs=(P("mkt", None), P(("mkt", "draw"), None, None), P()),
        check_vma=False,
    )
```

```python
import jax
import jax.numpy as jnp
from jax import lax
from jax.experimental import pallas as pl
from jax.experimental.pallas import tpu as pltpu
from jax.sharding import PartitionSpec as P

step_cap = 0.25
epsilon = 1e-06
LOG2E = 1.4426950408889634
VMEM = pl.BlockSpec(memory_space=pltpu.VMEM)
HBM = pl.BlockSpec(memory_space=pltpu.HBM)
SMEM = pl.BlockSpec(memory_space=pltpu.SMEM)
EVERY = ("mkt", "draw")


def pieces(value):
    high = value.astype(jnp.bfloat16).astype(jnp.float32)
    rest = value - high
    middle = rest.astype(jnp.bfloat16).astype(jnp.float32)
    return high, middle, rest - middle


def first_market(own):
    return lax.axis_index("draw") * own


def fill(ref, value):
    tile = jnp.broadcast_to(value, (8, ref.shape[1]))
    for row in range(0, ref.shape[0], 8):
        ref[row : row + 8, :] = tile


def column(value, slot, lanes=128):
    return jnp.broadcast_to(value[:, slot : slot + 1], (value.shape[0], lanes))


def share_columns(weights, raised_ref, own):
    slots, width = weights.shape
    draws = raised_ref.shape[2]
    lane = lax.broadcasted_iota(jnp.int32, (slots, width), 1)
    totals = jnp.ones((slots, width), jnp.float32)
    for m in range(own):
        weight = column(weights, m)
        total = jnp.zeros((slots, 128), jnp.float32)
        for g in range(0, draws, 128):
            raised = raised_ref[m, :, g : g + 128]
            below = 1.0 + jnp.sum(raised * weight, axis=0, keepdims=True)
            total = total + raised * (1.0 / below)
        totals = jnp.where(lane == m, jnp.sum(total, axis=1, keepdims=True), totals)
    return totals * weights * (1.0 / draws)


def contraction(state_ref, mean_util, raised_ref, own):
    log_share, usable = state_ref[0], state_ref[1] > 0.0
    weights = jnp.where(usable, jnp.exp(mean_util), 0.0)
    shares = share_columns(weights, raised_ref, own)
    return jnp.where(usable, log_share - jnp.log(jnp.where(usable, shares, 1.0)), 0.0)


def start_kernel(own, counts_hbm, sigma_hbm, log_share_hbm, x_hbm, nu_ref, raised_ref, state_ref, peak_ref, rows_ref, counts_ref, sigma_ref, log_share_ref, x_ref, sems):
    base = first_market(own)
    copies = [
        pltpu.make_async_copy(x_hbm.at[pl.ds(base, own)], x_ref, sems.at[0]),
        pltpu.make_async_copy(sigma_hbm, sigma_ref, sems.at[1]),
        pltpu.make_async_copy(log_share_hbm, log_share_ref, sems.at[2]),
        pltpu.make_async_copy(counts_hbm, counts_ref, sems.at[3]),
    ]
    for copy in copies:
        copy.start()
    for copy in copies:
        copy.wait()
    slots = log_share_ref.shape[1]
    depth = x_ref.shape[1]
    span = nu_ref.shape[2]
    level = lax.broadcasted_iota(jnp.int32, (depth, slots), 0)
    sigma = jnp.zeros((depth, slots), jnp.float32)
    for k in range(depth):
        sigma = jnp.where(level == k, sigma_ref[k], sigma)
    for m in range(own):
        high, middle, low = pieces(x_ref[m] * sigma * LOG2E)
        left = jnp.concatenate([high, high, middle, high, low, middle], axis=0)
        left = jnp.transpose(left).astype(jnp.bfloat16)
        for s in range(nu_ref.shape[0] // own):
            high, middle, low = pieces(nu_ref[s * own + m])
            right = jnp.concatenate([high, middle, high, low, high, middle], axis=0)
            tastes = jnp.dot(left, right.astype(jnp.bfloat16), preferred_element_type=jnp.float32)
            raised_ref[m, :, s * span : (s + 1) * span] = jnp.exp2(tastes)
    rows_ref[...] = jnp.zeros_like(rows_ref)
    for m in range(own):
        rows_ref[m : m + 1, 0:slots] = log_share_ref[pl.ds(base + m, 1), :]
    log_share = jnp.transpose(rows_ref[...])[0:slots, :]
    slot = lax.broadcasted_iota(jnp.int32, (slots, 8), 0)
    lane = lax.broadcasted_iota(jnp.int32, (slots, 8), 1)
    count = jnp.zeros((slots, 8), jnp.int32)
    for m in range(own):
        count = jnp.where(lane == m, counts_ref[base + m], count)
    usable = slot < count
    inside = jnp.sum(jnp.where(usable, jnp.exp(log_share), 0.0), axis=0, keepdims=True)
    mean_util = jnp.where(usable, log_share - jnp.log(1.0 - inside), 0.0)
    state_ref[0] = log_share
    state_ref[1] = jnp.where(usable, 1.0, 0.0)
    state_ref[2] = mean_util
    change = contraction(state_ref, mean_util, raised_ref, own)
    state_ref[3] = change
    state_ref[4] = jnp.zeros_like(change)
    fill(peak_ref, jnp.max(jnp.abs(change)))


def moved(peaks_ref, state_ref):
    largest = jnp.max(peaks_ref[...])
    step = jnp.minimum(1.0, step_cap / (largest + epsilon))
    return largest, state_ref[2] + step * state_ref[3]


def norm_row(turn, largest, state_ref):
    row = lax.broadcasted_iota(jnp.int32, state_ref.shape[1:], 0)
    return jnp.where(row == turn, largest, state_ref[4])


def as_rows(value):
    padded = jnp.concatenate([value, jnp.zeros((128 - value.shape[0], 8), jnp.float32)], axis=0)
    return jnp.transpose(padded)


def next_kernel(own, turn, peaks_ref, state_ref, raised_ref, out_ref, peak_ref, *rows_ref):
    largest, mean_util = moved(peaks_ref, state_ref)
    change = contraction(state_ref, mean_util, raised_ref, own)
    out_ref[0] = state_ref[0]
    out_ref[1] = state_ref[1]
    out_ref[2] = mean_util
    out_ref[3] = change
    out_ref[4] = norm_row(turn, largest, state_ref)
    fill(peak_ref, jnp.max(jnp.abs(change)))
    if rows_ref:
        rows_ref[0][0] = as_rows(mean_util)
        rows_ref[0][1] = as_rows(change)


def final_kernel(own, turn, draw_count, peaks_ref, state_ref, raised_hbm, *refs):
    rows_refs, (jacobian_ref, mean_ref, norms_ref, both_ref, raised_ref, sems) = refs[:draw_count], refs[draw_count:]

    def fetch(m):
        return pltpu.make_async_copy(raised_hbm.at[m], raised_ref.at[m], sems.at[m])

    for m in range(own):
        fetch(m).start()
    largest, mean_util = moved(peaks_ref, state_ref)
    step = jnp.minimum(1.0, step_cap / (largest + epsilon))
    norms = norm_row(turn, largest, state_ref)
    for t in range(turn + 1):
        norms_ref[t] = jnp.max(norms[t : t + 1, :])
    slots = mean_util.shape[0]
    draws = raised_ref.shape[2]
    mine = lax.axis_index("draw")
    for k in range(draw_count):
        rows = rows_refs[k][0] + step * rows_refs[k][1]
        first = (mine ^ k) * own
        for m in range(own):
            mean_ref[pl.ds(first + m, 1), :] = rows[m : m + 1, 0:slots]
    usable = state_ref[1]
    usable_rows = as_rows(usable)
    weights = jnp.where(usable > 0.0, jnp.exp(mean_util), 0.0)
    padding = jnp.zeros((64 - slots, 128), jnp.float32)
    row = lax.broadcasted_iota(jnp.int32, (slots, slots), 0)
    col = lax.broadcasted_iota(jnp.int32, (slots, slots), 1)
    identity = jnp.where(row == col, 1.0, 0.0)
    for m in range(own):
        weight = column(weights, m)
        total = jnp.zeros((slots, 128), jnp.float32)
        buffer = m % 2
        fetch(m).wait()
        for g in range(0, draws, 128):
            raised = raised_ref[m, :, g : g + 128] * weight
            chance = raised * (1.0 / (1.0 + jnp.sum(raised, axis=0, keepdims=True)))
            total = total + chance
            padded = jnp.concatenate([chance, padding], axis=0)
            high = padded.astype(jnp.bfloat16)
            low = (padded - high.astype(jnp.float32)).astype(jnp.bfloat16)
            both_ref[buffer, 0:64, g : g + 128] = high
            both_ref[buffer, 64:128, g : g + 128] = low
        product = lax.dot_general(
            both_ref[buffer, 0:64, :],
            both_ref[buffer],
            (((1,), (1,)), ((), ())),
            preferred_element_type=jnp.float32,
        )
        crossed = product[:, 64:128]
        cross = (product[:, 0:64] + crossed + jnp.transpose(crossed))[0:slots, 0:slots]
        shares = jnp.sum(total, axis=1, keepdims=True)
        valid = column(usable, m, slots) > 0.0
        paired = valid & (usable_rows[m : m + 1, 0:slots] > 0.0)
        divisor = jnp.where(valid, shares, 1.0)
        jacobian_ref[m] = jnp.where(paired, identity - cross / divisor, 0.0)


def in_hbm(array):
    return pltpu.with_memory_space_constraint(array, pltpu.HBM)


def params(mebibytes=16):
    return pltpu.CompilerParams(vmem_limit_bytes=mebibytes << 20)


def shards(x_char, nu_draws, coef_sigma, log_share, counts):
    markets, slots = log_share.shape
    depth, span = nu_draws.shape[1:]
    draw_count, every = lax.axis_size("draw"), lax.axis_size(EVERY)
    own = markets // draw_count
    f32 = jnp.float32
    raised_shape = jax.ShapeDtypeStruct((own, slots, span * draw_count), f32)
    state_shape = jax.ShapeDtypeStruct((5, slots, 8), f32)
    peak_shape = jax.ShapeDtypeStruct((every, 128), f32)

    def everywhere(peak):
        return lax.all_to_all(peak.reshape(every, 1, 128), EVERY, 0, 0, tiled=True).reshape(every, 128)

    nu_own = lax.all_to_all(nu_draws, "draw", 0, 0, tiled=True)
    raised, state, peak = pl.pallas_call(
        lambda *refs: start_kernel(own, *refs),
        out_shape=(raised_shape, state_shape, peak_shape),
        in_specs=[HBM, HBM, HBM, HBM, VMEM],
        out_specs=(VMEM, VMEM, VMEM),
        scratch_shapes=[
            pltpu.VMEM((8, 128), f32),
            pltpu.SMEM((markets,), jnp.int32),
            pltpu.SMEM((depth,), f32),
            pltpu.VMEM((markets, slots), f32),
            pltpu.VMEM((own, depth, slots), f32),
            pltpu.SemaphoreType.DMA((4,)),
        ],
        compiler_params=params(),
        name="start",
    )(*map(in_hbm, (counts, coef_sigma, log_share, jnp.transpose(x_char, (0, 2, 1)))), nu_own)
    rows_shape = jax.ShapeDtypeStruct((2, 8, 128), f32)
    for turn in range(2):
        outs = (state_shape, peak_shape) + (() if turn == 0 else (rows_shape,))
        state, peak, *rows = pl.pallas_call(
            lambda *refs, turn=turn: next_kernel(own, turn, *refs),
            out_shape=outs,
            in_specs=[VMEM, VMEM, VMEM],
            out_specs=tuple(VMEM for _ in outs),
            compiler_params=params(),
            name="next",
        )(everywhere(peak), state, raised)
    peaks = everywhere(peak)
    rows += [
        lax.ppermute(rows[0], "draw", [(d, d ^ k) for d in range(draw_count)]) for k in range(1, draw_count)
    ]
    jacobian, mean_util, norms = pl.pallas_call(
        lambda *refs: final_kernel(own, 2, draw_count, *refs),
        out_shape=(
            jax.ShapeDtypeStruct((own, slots, slots), f32),
            jax.ShapeDtypeStruct((markets, slots), f32),
            jax.ShapeDtypeStruct((3,), f32),
        ),
        in_specs=[VMEM, VMEM, HBM] + [VMEM] * draw_count,
        out_specs=(VMEM, VMEM, SMEM),
        scratch_shapes=[
            pltpu.VMEM((2, 128, span * draw_count), jnp.bfloat16),
            pltpu.VMEM((own, slots, span * draw_count), f32),
            pltpu.SemaphoreType.DMA((own,)),
        ],
        compiler_params=params(),
        name="final",
    )(peaks, state, in_hbm(raised), *rows)
    return (mean_util, jacobian, norms)


def solution(mesh):
    return jax.shard_map(
        shards,
        mesh=mesh,
        in_specs=(P("mkt", None, None), P("mkt", None, "draw"), P(), P("mkt", None), P("mkt")),
        out_specs=(P("mkt", None), P(("mkt", "draw"), None, None), P()),
        check_vma=False,
    )
```

```python
import jax
import jax.numpy as jnp
from jax import lax
from jax.experimental import pallas as pl
from jax.experimental.pallas import tpu as pltpu
from jax.sharding import PartitionSpec as P

step_cap = 0.25
epsilon = 1e-06
LOG2E = 1.4426950408889634
VMEM = pl.BlockSpec(memory_space=pltpu.VMEM)
HBM = pl.BlockSpec(memory_space=pltpu.HBM)
SMEM = pl.BlockSpec(memory_space=pltpu.SMEM)


def pieces(value):
    high = value.astype(jnp.bfloat16).astype(jnp.float32)
    rest = value - high
    middle = rest.astype(jnp.bfloat16).astype(jnp.float32)
    return high, middle, rest - middle


def in_hbm(array):
    return pltpu.with_memory_space_constraint(array, pltpu.HBM)


def params(mebibytes=16):
    return pltpu.CompilerParams(vmem_limit_bytes=mebibytes << 20)


def column(value, slot, lanes=128):
    return jnp.broadcast_to(value[:, slot : slot + 1], (value.shape[0], lanes))


def fill(ref, value):
    tile = jnp.broadcast_to(value, (8, ref.shape[1]))
    for row in range(0, ref.shape[0], 8):
        ref[row : row + 8, :] = tile


def turned(value):
    rows = value.shape[0]
    return jnp.transpose(jnp.concatenate([value, jnp.zeros((128 - rows, 128), jnp.float32)], axis=0))


def both_starts(copies):
    for copy in copies:
        copy.start()
    return copies


def sigma_levels(sigma_ref, depth, slots):
    level = lax.broadcasted_iota(jnp.int32, (depth, slots), 0)
    sigma = jnp.zeros((depth, slots), jnp.float32)
    for k in range(depth):
        sigma = jnp.where(level == k, sigma_ref[k], sigma)
    return sigma * LOG2E


def left_side(scaled):
    high, middle, low = pieces(scaled)
    left = jnp.concatenate([high, high, middle, high, low, middle], axis=0)
    return jnp.transpose(left).astype(jnp.bfloat16)


def raise_tastes(left, draws):
    high, middle, low = pieces(draws)
    right = jnp.concatenate([high, middle, high, low, high, middle], axis=0)
    return jnp.exp2(jnp.dot(left, right.astype(jnp.bfloat16), preferred_element_type=jnp.float32))


def usable_weights(state_ref, mean_util):
    return jnp.where(state_ref[1] > 0.0, jnp.exp(mean_util), 0.0)


def share_sums(weights, raised_ref):
    markets, slots, draws = raised_ref.shape
    lane = lax.broadcasted_iota(jnp.int32, (32, 128), 1)
    sums = jnp.zeros((32, 128), jnp.float32)
    upper = jnp.zeros((32, 128), jnp.float32)
    for m in range(markets):
        weight = column(weights, m)
        total = jnp.zeros((slots, 128), jnp.float32)
        for g in range(0, draws, 128):
            raised = raised_ref[m, :, g : g + 128]
            below = 1.0 + jnp.sum(raised * weight, axis=0, keepdims=True)
            total = total + raised * (1.0 / below)
        one = jnp.sum(total, axis=1, keepdims=True)
        rest = jnp.concatenate([one[32:slots], jnp.zeros((64 - slots, 1), jnp.float32)], axis=0)
        sums = jnp.where(lane == m, one[0:32], sums)
        upper = jnp.where(lane == m + 64, rest, upper)
    return jnp.where(lane < 64, sums, upper)


def send_copies(sums_ref, sums):
    for d in range(sums_ref.shape[0]):
        sums_ref[d] = sums


def start_kernel(counts_hbm, sigma_hbm, log_share_hbm, x_hbm, nu_hbm, raised_ref, state_ref, sums_ref, counts_ref, sigma_ref, rows_ref, log_share_ref, x_ref, nu_ref, sems):
    markets, slots = log_share_hbm.shape
    depth = x_hbm.shape[1]
    chunk = markets // 4
    small = both_starts(
        [
            pltpu.make_async_copy(x_hbm, x_ref, sems.at[0]),
            pltpu.make_async_copy(sigma_hbm, sigma_ref, sems.at[1]),
            pltpu.make_async_copy(log_share_hbm, log_share_ref, sems.at[2]),
            pltpu.make_async_copy(counts_hbm, counts_ref, sems.at[3]),
        ]
    )
    large = both_starts(
        [
            pltpu.make_async_copy(nu_hbm.at[pl.ds(c * chunk, chunk)], nu_ref.at[pl.ds(c * chunk, chunk)], sems.at[4 + c])
            for c in range(4)
        ]
    )
    rows_ref[...] = jnp.zeros_like(rows_ref)
    for copy in small:
        copy.wait()
    sigma = sigma_levels(sigma_ref, depth, slots)
    for m in range(markets):
        if m % chunk == 0:
            large[m // chunk].wait()
        raised_ref[m] = raise_tastes(left_side(x_ref[m] * sigma), nu_ref[m])
    rows_ref[0:markets, 0:slots] = log_share_ref[...]
    log_share = jnp.transpose(rows_ref[...])[0:slots, :]
    slot = lax.broadcasted_iota(jnp.int32, (slots, 128), 0)
    lane = lax.broadcasted_iota(jnp.int32, (8, 128), 1)
    count = jnp.zeros((8, 128), jnp.int32)
    for m in range(markets):
        count = jnp.where(lane == m, counts_ref[m], count)
    usable = slot < jnp.broadcast_to(count[0:1, :], (slots, 128))
    inside = jnp.sum(jnp.where(usable, jnp.exp(log_share), 0.0), axis=0, keepdims=True)
    mean_util = jnp.where(usable, log_share - jnp.log(1.0 - inside), 0.0)
    state_ref[0] = log_share
    state_ref[1] = jnp.where(usable, 1.0, 0.0)
    state_ref[2] = mean_util
    state_ref[3] = jnp.zeros_like(mean_util)
    send_copies(sums_ref, share_sums(usable_weights(state_ref, mean_util), raised_ref))


def change_kernel(inverse, sums_ref, state_ref, change_ref, peak_ref):
    total = sums_ref[0]
    for d in range(1, sums_ref.shape[0]):
        total = total + sums_ref[d]
    slots = change_ref.shape[0]
    sums = jnp.concatenate([total, pltpu.roll(total, 64, axis=1)[0 : slots - 32]], axis=0)
    usable = state_ref[1] > 0.0
    shares = sums * usable_weights(state_ref, state_ref[2]) * inverse
    change = jnp.where(usable, state_ref[0] - jnp.log(jnp.where(usable, shares, 1.0)), 0.0)
    change_ref[...] = change
    fill(peak_ref, jnp.max(jnp.abs(change)))


def moved(turn, peaks_ref, state_ref, change_ref):
    largest = jnp.max(peaks_ref[...])
    step = jnp.minimum(1.0, step_cap / (largest + epsilon))
    row = lax.broadcasted_iota(jnp.int32, change_ref.shape, 0)
    return state_ref[2] + step * change_ref[...], jnp.where(row == turn, largest, state_ref[3])


def next_kernel(turn, peaks_ref, state_ref, change_ref, raised_ref, out_ref, sums_ref):
    mean_util, norms = moved(turn, peaks_ref, state_ref, change_ref)
    out_ref[0] = state_ref[0]
    out_ref[1] = state_ref[1]
    out_ref[2] = mean_util
    out_ref[3] = norms
    send_copies(sums_ref, share_sums(usable_weights(state_ref, mean_util), raised_ref))


def sending_kernel(turn, own, peaks_ref, state_ref, change_ref, raised_ref, nu_hbm, partner_ref, out_ref, sums_ref, *refs):
    sends, sems = refs[:-1], refs[-1]
    mine = lax.axis_index("draw")
    copies = []
    for k, send in enumerate(sends):
        first = (mine ^ (2 * (k + 1))) * own
        copies.append(pltpu.make_async_copy(nu_hbm.at[pl.ds(first, own)], send.at[0], sems.at[k]))
        for m in range(own):
            send[1, m] = partner_ref[first + m]
    both_starts(copies)
    next_kernel(turn, peaks_ref, state_ref, change_ref, raised_ref, out_ref, sums_ref)
    for copy in copies:
        copy.wait()


def final_kernel(turn, own, peaks_ref, state_ref, change_ref, x_hbm, sigma_hbm, nu_hbm, partner_ref, *refs):
    received = refs[:3]
    jacobian_ref, mean_ref, norms_ref, raised_ref, both_ref, x_ref, sigma_ref, nu_ref, sems = refs[3:]
    base = lax.axis_index("draw") * own
    copies = both_starts(
        [
            pltpu.make_async_copy(x_hbm.at[pl.ds(base, own)], x_ref, sems.at[0]),
            pltpu.make_async_copy(sigma_hbm, sigma_ref, sems.at[1]),
            pltpu.make_async_copy(nu_hbm.at[pl.ds(base, own)], nu_ref, sems.at[2]),
        ]
    )
    mean_util, norms = moved(turn, peaks_ref, state_ref, change_ref)
    for t in range(turn + 1):
        norms_ref[t] = jnp.max(norms[t : t + 1, :])
    slots = mean_util.shape[0]
    markets = mean_ref.shape[0]
    mean_ref[...] = turned(mean_util)[0:markets, 0:slots]
    shift = 128 - base
    usable = pltpu.roll(state_ref[1], shift, axis=1)
    weights = pltpu.roll(usable_weights(state_ref, mean_util), shift, axis=1)
    usable_rows = turned(usable)
    for copy in copies:
        copy.wait()
    sources = [nu_ref, partner_ref.at[pl.ds(base, own)]]
    for ref in received:
        sources += [ref.at[0], ref.at[1]]
    span = nu_ref.shape[2]
    draws = span * len(sources)
    sigma = sigma_levels(sigma_ref, x_ref.shape[1], slots)
    for m in range(own):
        left = left_side(x_ref[m] * sigma)
        for s, source in enumerate(sources):
            raised_ref[m, :, s * span : (s + 1) * span] = raise_tastes(left, source[m])
    padding = jnp.zeros((64 - slots, 128), jnp.float32)
    row = lax.broadcasted_iota(jnp.int32, (slots, slots), 0)
    col = lax.broadcasted_iota(jnp.int32, (slots, slots), 1)
    identity = jnp.where(row == col, 1.0, 0.0)
    for m in range(own):
        weight = column(weights, m)
        total = jnp.zeros((slots, 128), jnp.float32)
        buffer = m % 2
        for g in range(0, draws, 128):
            raised = raised_ref[m, :, g : g + 128] * weight
            chance = raised * (1.0 / (1.0 + jnp.sum(raised, axis=0, keepdims=True)))
            total = total + chance
            padded = jnp.concatenate([chance, padding], axis=0)
            high = padded.astype(jnp.bfloat16)
            low = (padded - high.astype(jnp.float32)).astype(jnp.bfloat16)
            both_ref[buffer, 0:64, g : g + 128] = high
            both_ref[buffer, 64:128, g : g + 128] = low
        product = lax.dot_general(
            both_ref[buffer, 0:64, :],
            both_ref[buffer],
            (((1,), (1,)), ((), ())),
            preferred_element_type=jnp.float32,
        )
        crossed = product[:, 64:128]
        cross = (product[:, 0:64] + crossed + jnp.transpose(crossed))[0:slots, 0:slots]
        shares = jnp.sum(total, axis=1, keepdims=True)
        valid = column(usable, m, slots) > 0.0
        paired = valid & (usable_rows[m : m + 1, 0:slots] > 0.0)
        divisor = jnp.where(valid, shares, 1.0)
        jacobian_ref[m] = jnp.where(paired, identity - cross / divisor, 0.0)


def shards(x_char, nu_draws, coef_sigma, log_share, counts):
    markets, slots = log_share.shape
    depth, span = nu_draws.shape[1:]
    draw_count, mkt_count = lax.axis_size("draw"), lax.axis_size("mkt")
    own = markets // draw_count
    draws = span * draw_count
    f32 = jnp.float32
    state_shape = jax.ShapeDtypeStruct((4, slots, 128), f32)
    sums_shape = jax.ShapeDtypeStruct((draw_count, 32, 128), f32)
    change_shape = jax.ShapeDtypeStruct((slots, 128), f32)
    peak_shape = jax.ShapeDtypeStruct((mkt_count, 128), f32)
    send_shape = jax.ShapeDtypeStruct((2, own, depth, span), f32)

    def exchange(array, axis, distance):
        return lax.ppermute(array, axis, [(d, d ^ distance) for d in range(lax.axis_size(axis))])

    def changed(sums, state):
        change, peak = pl.pallas_call(
            lambda *refs: change_kernel(1.0 / draws, *refs),
            out_shape=(change_shape, peak_shape),
            in_specs=[VMEM, VMEM],
            out_specs=(VMEM, VMEM),
            compiler_params=params(),
            name="change",
        )(lax.all_to_all(sums, "draw", 0, 0, tiled=True), state)
        peaks = lax.all_to_all(peak.reshape(mkt_count, 1, 128), "mkt", 0, 0, tiled=True)
        return change, peaks.reshape(mkt_count, 128)

    partner = exchange(nu_draws, "draw", 1)
    x_rows = in_hbm(jnp.transpose(x_char, (0, 2, 1)))
    raised, state, sums = pl.pallas_call(
        start_kernel,
        out_shape=(jax.ShapeDtypeStruct((markets, slots, span), f32), state_shape, sums_shape),
        in_specs=[HBM] * 5,
        out_specs=(VMEM, VMEM, VMEM),
        scratch_shapes=[
            pltpu.SMEM((markets,), jnp.int32),
            pltpu.SMEM((depth,), f32),
            pltpu.VMEM((128, 128), f32),
            pltpu.VMEM((markets, slots), f32),
            pltpu.VMEM((markets, depth, slots), f32),
            pltpu.VMEM((markets, depth, span), f32),
            pltpu.SemaphoreType.DMA((8,)),
        ],
        compiler_params=params(),
        name="start",
    )(in_hbm(counts), in_hbm(coef_sigma), in_hbm(log_share), x_rows, in_hbm(nu_draws))
    change, peaks = changed(sums, state)
    state, sums = pl.pallas_call(
        lambda *refs: next_kernel(0, *refs),
        out_shape=(state_shape, sums_shape),
        in_specs=[VMEM] * 4,
        out_specs=(VMEM, VMEM),
        compiler_params=params(),
        name="next",
    )(peaks, state, change, raised)
    change, peaks = changed(sums, state)
    state, sums, *sends = pl.pallas_call(
        lambda *refs: sending_kernel(1, own, *refs),
        out_shape=(state_shape, sums_shape) + (send_shape,) * 3,
        in_specs=[VMEM] * 4 + [HBM, VMEM],
        out_specs=(VMEM,) * 5,
        scratch_shapes=[pltpu.SemaphoreType.DMA((3,))],
        compiler_params=params(),
        name="sending",
    )(peaks, state, change, raised, in_hbm(nu_draws), partner)
    received = [exchange(send, "draw", 2 * (k + 1)) for k, send in enumerate(sends)]
    change, peaks = changed(sums, state)
    jacobian, mean_util, norms = pl.pallas_call(
        lambda *refs: final_kernel(2, own, *refs),
        out_shape=(
            jax.ShapeDtypeStruct((own, slots, slots), f32),
            jax.ShapeDtypeStruct((markets, slots), f32),
            jax.ShapeDtypeStruct((3,), f32),
        ),
        in_specs=[VMEM] * 3 + [HBM] * 3 + [VMEM] * 4,
        out_specs=(VMEM, VMEM, SMEM),
        scratch_shapes=[
            pltpu.VMEM((own, slots, draws), f32),
            pltpu.VMEM((2, 128, draws), jnp.bfloat16),
            pltpu.VMEM((own, depth, slots), f32),
            pltpu.SMEM((depth,), f32),
            pltpu.VMEM((own, depth, span), f32),
            pltpu.SemaphoreType.DMA((3,)),
        ],
        compiler_params=params(),
        name="final",
    )(peaks, state, change, x_rows, in_hbm(coef_sigma), in_hbm(nu_draws), partner, *received)
    return (mean_util, jacobian, norms)


def solution(mesh):
    return jax.shard_map(
        shards,
        mesh=mesh,
        in_specs=(P("mkt", None, None), P("mkt", None, "draw"), P(), P("mkt", None), P("mkt")),
        out_specs=(P("mkt", None), P(("mkt", "draw"), None, None), P()),
        check_vma=False,
    )
```

```python
import jax
import jax.numpy as jnp
from jax import lax
from jax.experimental import pallas as pl
from jax.experimental.pallas import tpu as pltpu
from jax.sharding import PartitionSpec as P

step_cap = 0.25
epsilon = 1e-06
LOG2E = 1.4426950408889634
VMEM = pl.BlockSpec(memory_space=pltpu.VMEM)
HBM = pl.BlockSpec(memory_space=pltpu.HBM)
SMEM = pl.BlockSpec(memory_space=pltpu.SMEM)
EVERY = ("mkt", "draw")


def pieces(value):
    high = value.astype(jnp.bfloat16).astype(jnp.float32)
    rest = value - high
    middle = rest.astype(jnp.bfloat16).astype(jnp.float32)
    return high, middle, rest - middle


def in_hbm(array):
    return pltpu.with_memory_space_constraint(array, pltpu.HBM)


def params(mebibytes=16):
    return pltpu.CompilerParams(vmem_limit_bytes=mebibytes << 20)


def column(value, slot, lanes=128):
    return jnp.broadcast_to(value[:, slot : slot + 1], (value.shape[0], lanes))


def fill(ref, value):
    tile = jnp.broadcast_to(value, (8, ref.shape[1]))
    for row in range(0, ref.shape[0], 8):
        ref[row : row + 8, :] = tile


def turned(value):
    rows = value.shape[0]
    return jnp.transpose(jnp.concatenate([value, jnp.zeros((128 - rows, 128), jnp.float32)], axis=0))


def both_starts(copies):
    for copy in copies:
        copy.start()
    return copies


def sigma_levels(sigma_ref, depth, slots):
    level = lax.broadcasted_iota(jnp.int32, (depth, slots), 0)
    sigma = jnp.zeros((depth, slots), jnp.float32)
    for k in range(depth):
        sigma = jnp.where(level == k, sigma_ref[k], sigma)
    return sigma * LOG2E


def left_side(scaled):
    high, middle, low = pieces(scaled)
    left = jnp.concatenate([high, high, middle, high, low, middle], axis=0)
    return jnp.transpose(left).astype(jnp.bfloat16)


def raise_tastes(left, draws):
    high, middle, low = pieces(draws)
    right = jnp.concatenate([high, middle, high, low, high, middle], axis=0)
    return jnp.exp2(jnp.dot(left, right.astype(jnp.bfloat16), preferred_element_type=jnp.float32))


def usable_weights(state_ref, mean_util):
    return jnp.where(state_ref[1] > 0.0, jnp.exp(mean_util), 0.0)


def send_copies(sums_ref, sums):
    for d in range(sums_ref.shape[0]):
        sums_ref[d] = sums


def weight_columns(weights, columns_ref):
    for m in range(columns_ref.shape[0]):
        columns_ref[m] = column(weights, m)


def totals_over(columns_ref, raised_ref):
    markets, slots, draws = raised_ref.shape
    for m in range(markets):
        weight = columns_ref[m]
        total = jnp.zeros((slots, 128), jnp.float32)
        for g in range(0, draws, 128):
            raised = raised_ref[m, :, g : g + 128]
            below = 1.0 + jnp.sum(raised * weight, axis=0, keepdims=True)
            total = total + raised * (1.0 / below)
        columns_ref[m] = total


def packed_sums(totals_ref):
    markets, slots = totals_ref.shape[:2]
    lane = lax.broadcasted_iota(jnp.int32, (32, 128), 1)
    sums = jnp.zeros((32, 128), jnp.float32)
    upper = jnp.zeros((32, 128), jnp.float32)
    for m in range(markets):
        one = jnp.sum(totals_ref[m], axis=1, keepdims=True)
        rest = jnp.concatenate([one[32:slots], jnp.zeros((64 - slots, 1), jnp.float32)], axis=0)
        sums = jnp.where(lane == m, one[0:32], sums)
        upper = jnp.where(lane == m + 64, rest, upper)
    return jnp.where(lane < 64, sums, upper)


def start_kernel(counts_hbm, sigma_hbm, log_share_hbm, x_hbm, nu_hbm, state_ref, sums_ref, nu_ref, counts_ref, sigma_ref, rows_ref, log_share_ref, x_ref, left_ref, raised_ref, columns_ref, sems):
    markets, slots = log_share_hbm.shape
    depth = x_hbm.shape[1]
    chunk = markets // 4
    small = both_starts(
        [
            pltpu.make_async_copy(x_hbm, x_ref, sems.at[0]),
            pltpu.make_async_copy(sigma_hbm, sigma_ref, sems.at[1]),
            pltpu.make_async_copy(log_share_hbm, log_share_ref, sems.at[2]),
            pltpu.make_async_copy(counts_hbm, counts_ref, sems.at[3]),
        ]
    )
    large = both_starts(
        [
            pltpu.make_async_copy(nu_hbm.at[pl.ds(c * chunk, chunk)], nu_ref.at[pl.ds(c * chunk, chunk)], sems.at[4 + c])
            for c in range(4)
        ]
    )
    rows_ref[...] = jnp.zeros_like(rows_ref)
    for copy in small:
        copy.wait()
    sigma = sigma_levels(sigma_ref, depth, slots)
    for m in range(markets):
        left_ref[m] = left_side(x_ref[m] * sigma)
    rows_ref[0:markets, 0:slots] = log_share_ref[...]
    log_share = jnp.transpose(rows_ref[...])[0:slots, :]
    slot = lax.broadcasted_iota(jnp.int32, (slots, 128), 0)
    lane = lax.broadcasted_iota(jnp.int32, (8, 128), 1)
    count = jnp.zeros((8, 128), jnp.int32)
    for m in range(markets):
        count = jnp.where(lane == m, counts_ref[m], count)
    usable = slot < jnp.broadcast_to(count[0:1, :], (slots, 128))
    inside = jnp.sum(jnp.where(usable, jnp.exp(log_share), 0.0), axis=0, keepdims=True)
    mean_util = jnp.where(usable, log_share - jnp.log(1.0 - inside), 0.0)
    state_ref[0] = log_share
    state_ref[1] = jnp.where(usable, 1.0, 0.0)
    state_ref[2] = mean_util
    weight_columns(jnp.where(usable, jnp.exp(mean_util), 0.0), columns_ref)
    for copy in large:
        copy.wait()
    for m in range(markets):
        raised_ref[m] = raise_tastes(left_ref[m], nu_ref[m])
    totals_over(columns_ref, raised_ref)
    send_copies(sums_ref, packed_sums(columns_ref))


def change_kernel(inverse, sums_ref, all_ref, nu_ref, partner_ref, state_ref, peak_ref, *sends):
    own = sends[0].shape[1]
    mine = lax.axis_index("draw")
    for k, send in enumerate(sends):
        first = (mine ^ (2 * (k + 1))) * own
        for m in range(own):
            send[0, m] = nu_ref[first + m]
            send[1, m] = partner_ref[first + m]
    total = sums_ref[0]
    for d in range(1, sums_ref.shape[0]):
        total = total + sums_ref[d]
    slots = all_ref.shape[1]
    sums = jnp.concatenate([total, pltpu.roll(total, 64, axis=1)[0 : slots - 32]], axis=0)
    usable = all_ref[1] > 0.0
    shares = sums * usable_weights(all_ref, all_ref[2]) * inverse
    change = jnp.where(usable, all_ref[0] - jnp.log(jnp.where(usable, shares, 1.0)), 0.0)
    fill(peak_ref, jnp.max(jnp.abs(change)))
    kept = lax.broadcasted_iota(jnp.int32, (slots, 8), 1) < own
    for p, plane in enumerate((all_ref[0], all_ref[1], all_ref[2], change)):
        state_ref[p] = jnp.where(kept, pltpu.roll(plane, 128 - mine * own, axis=1)[:, 0:8], 0.0)
    state_ref[4] = jnp.zeros((slots, 8), jnp.float32)


def moved(turn, peaks_ref, state_ref):
    largest = jnp.max(peaks_ref[...])
    step = jnp.minimum(1.0, step_cap / (largest + epsilon))
    row = lax.broadcasted_iota(jnp.int32, state_ref.shape[1:], 0)
    return step, state_ref[2] + step * state_ref[3], jnp.where(row == turn, largest, state_ref[4])


def next_change(turn, peaks_ref, state_ref, out_ref, raised_ref, columns_ref):
    own, slots, draws = raised_ref.shape
    _, mean_util, norms = moved(turn, peaks_ref, state_ref)
    usable = state_ref[1] > 0.0
    weights = jnp.where(usable, jnp.exp(mean_util), 0.0)
    weight_columns(weights, columns_ref)
    totals_over(columns_ref, raised_ref)
    lane = lax.broadcasted_iota(jnp.int32, weights.shape, 1)
    sums = jnp.ones(weights.shape, jnp.float32)
    for m in range(own):
        sums = jnp.where(lane == m, jnp.sum(columns_ref[m], axis=1, keepdims=True), sums)
    shares = sums * weights * (1.0 / draws)
    change = jnp.where(usable, state_ref[0] - jnp.log(jnp.where(usable, shares, 1.0)), 0.0)
    out_ref[0] = state_ref[0]
    out_ref[1] = state_ref[1]
    out_ref[2] = mean_util
    out_ref[3] = change
    out_ref[4] = norms
    return mean_util, change


def second_kernel(peaks_ref, state_ref, x_hbm, sigma_hbm, nu_hbm, partner_ref, *refs):
    received = refs[:3]
    raised_ref, out_ref, peak_ref, x_ref, sigma_ref, nu_ref, left_ref, columns_ref, sems = refs[3:]
    own, slots, draws = raised_ref.shape
    base = lax.axis_index("draw") * own
    copies = both_starts(
        [
            pltpu.make_async_copy(x_hbm.at[pl.ds(base, own)], x_ref, sems.at[0]),
            pltpu.make_async_copy(sigma_hbm, sigma_ref, sems.at[1]),
            pltpu.make_async_copy(nu_hbm.at[pl.ds(base, own)], nu_ref, sems.at[2]),
        ]
    )
    for copy in copies:
        copy.wait()
    sources = [nu_ref, partner_ref.at[pl.ds(base, own)]]
    for ref in received:
        sources += [ref.at[0], ref.at[1]]
    span = nu_ref.shape[2]
    sigma = sigma_levels(sigma_ref, x_ref.shape[1], slots)
    for m in range(own):
        left_ref[m] = left_side(x_ref[m] * sigma)
    for m in range(own):
        for s, source in enumerate(sources):
            raised_ref[m, :, s * span : (s + 1) * span] = raise_tastes(left_ref[m], source[m])
    _, change = next_change(0, peaks_ref, state_ref, out_ref, raised_ref, columns_ref)
    fill(peak_ref, jnp.max(jnp.abs(change)))


def as_rows(value):
    padded = jnp.concatenate([value, jnp.zeros((128 - value.shape[0], 8), jnp.float32)], axis=0)
    return jnp.transpose(padded)


def third_kernel(peaks_ref, state_ref, raised_ref, out_ref, rows_ref, columns_ref):
    mean_util, change = next_change(1, peaks_ref, state_ref, out_ref, raised_ref, columns_ref)
    send_copies(rows_ref, jnp.concatenate([as_rows(mean_util), as_rows(change)], axis=0))


def join_kernel(rows_ref, peak_ref):
    largest = jnp.abs(rows_ref[0, 8:16, :])
    for d in range(1, rows_ref.shape[0]):
        largest = jnp.maximum(largest, jnp.abs(rows_ref[d, 8:16, :]))
    fill(peak_ref, jnp.max(largest))


def final_kernel(peaks_ref, state_ref, rows_ref, raised_ref, jacobian_ref, mean_ref, norms_ref, both_ref, columns_ref, product_ref):
    own, slots, draws = raised_ref.shape
    step, mean_util, norms = moved(2, peaks_ref, state_ref)
    usable = state_ref[1]
    weight_columns(jnp.where(usable > 0.0, jnp.exp(mean_util), 0.0), columns_ref)
    usable_rows = as_rows(usable)
    for t in range(3):
        norms_ref[t] = jnp.max(norms[t : t + 1, :])
    for d in range(rows_ref.shape[0]):
        rows = rows_ref[d, 0:8, :] + step * rows_ref[d, 8:16, :]
        mean_ref[d * own : (d + 1) * own, :] = rows[0:own, 0:slots]
    padding = jnp.zeros((64 - slots, 128), jnp.float32)
    for m in range(own):
        weight = columns_ref[m]
        total = jnp.zeros((slots, 128), jnp.float32)
        buffer = m % 2
        for g in range(0, draws, 128):
            raised = raised_ref[m, :, g : g + 128] * weight
            chance = raised * (1.0 / (1.0 + jnp.sum(raised, axis=0, keepdims=True)))
            total = total + chance
            padded = jnp.concatenate([chance, padding], axis=0)
            high = padded.astype(jnp.bfloat16)
            low = (padded - high.astype(jnp.float32)).astype(jnp.bfloat16)
            both_ref[buffer, 0:64, g : g + 128] = high
            both_ref[buffer, 64:128, g : g + 128] = low
        columns_ref[m] = total
        product_ref[m] = lax.dot_general(
            both_ref[buffer, 0:64, :],
            both_ref[buffer],
            (((1,), (1,)), ((), ())),
            preferred_element_type=jnp.float32,
        )
    row = lax.broadcasted_iota(jnp.int32, (slots, slots), 0)
    col = lax.broadcasted_iota(jnp.int32, (slots, slots), 1)
    identity = jnp.where(row == col, 1.0, 0.0)
    for m in range(own):
        product = product_ref[m]
        crossed = product[:, 64:128]
        cross = (product[:, 0:64] + crossed + jnp.transpose(crossed))[0:slots, 0:slots]
        shares = jnp.sum(columns_ref[m], axis=1, keepdims=True)
        valid = column(usable, m, slots) > 0.0
        paired = valid & (usable_rows[m : m + 1, 0:slots] > 0.0)
        divisor = jnp.where(valid, shares, 1.0)
        jacobian_ref[m] = jnp.where(paired, identity - cross / divisor, 0.0)


def shards(x_char, nu_draws, coef_sigma, log_share, counts):
    markets, slots = log_share.shape
    depth, span = nu_draws.shape[1:]
    draw_count, mkt_count, every = (lax.axis_size(axis) for axis in ("draw", "mkt", EVERY))
    own = markets // draw_count
    draws = span * draw_count
    f32, bf16 = jnp.float32, jnp.bfloat16
    shape = lambda *sizes: jax.ShapeDtypeStruct(sizes, f32)
    state_shape = shape(5, slots, 8)
    columns = pltpu.VMEM((own, slots, 128), f32)

    def exchange(array, distance):
        return lax.ppermute(array, "draw", [(d, d ^ distance) for d in range(draw_count)])

    def peaks_of(peak, axis):
        count = peak.shape[0]
        return lax.all_to_all(peak.reshape(count, 1, 128), axis, 0, 0, tiled=True).reshape(count, 128)

    partner = exchange(nu_draws, 1)
    x_rows, sigma, nu_hbm = in_hbm(jnp.transpose(x_char, (0, 2, 1))), in_hbm(coef_sigma), in_hbm(nu_draws)
    all_state, sums, nu_near = pl.pallas_call(
        start_kernel,
        out_shape=(shape(3, slots, 128), shape(draw_count, 32, 128), shape(markets, depth, span)),
        in_specs=[HBM] * 5,
        out_specs=(VMEM,) * 3,
        scratch_shapes=[
            pltpu.SMEM((markets,), jnp.int32),
            pltpu.SMEM((depth,), f32),
            pltpu.VMEM((128, 128), f32),
            pltpu.VMEM((markets, slots), f32),
            pltpu.VMEM((markets, depth, slots), f32),
            pltpu.VMEM((markets, slots, 6 * depth), bf16),
            pltpu.VMEM((markets, slots, span), f32),
            pltpu.VMEM((markets, slots, 128), f32),
            pltpu.SemaphoreType.DMA((8,)),
        ],
        compiler_params=params(),
        name="start",
    )(in_hbm(counts), sigma, in_hbm(log_share), x_rows, nu_hbm)
    state, peak, *sends = pl.pallas_call(
        lambda *refs: change_kernel(1.0 / draws, *refs),
        out_shape=(state_shape, shape(mkt_count, 128)) + (shape(2, own, depth, span),) * 3,
        in_specs=[VMEM] * 4,
        out_specs=(VMEM,) * 5,
        compiler_params=params(),
        name="change",
    )(lax.all_to_all(sums, "draw", 0, 0, tiled=True), all_state, nu_near, partner)
    peaks = peaks_of(peak, "mkt")
    received = [exchange(send, 2 * (k + 1)) for k, send in enumerate(sends)]
    raised, state, peak = pl.pallas_call(
        second_kernel,
        out_shape=(shape(own, slots, draws), state_shape, shape(every, 128)),
        in_specs=[VMEM] * 2 + [HBM] * 3 + [VMEM] * 4,
        out_specs=(VMEM,) * 3,
        scratch_shapes=[
            pltpu.VMEM((own, depth, slots), f32),
            pltpu.SMEM((depth,), f32),
            pltpu.VMEM((own, depth, span), f32),
            pltpu.VMEM((own, slots, 6 * depth), bf16),
            columns,
            pltpu.SemaphoreType.DMA((3,)),
        ],
        compiler_params=params(),
        name="second",
    )(peaks, state, x_rows, sigma, nu_hbm, partner, *received)
    state, rows = pl.pallas_call(
        third_kernel,
        out_shape=(state_shape, shape(draw_count, 16, 128)),
        in_specs=[VMEM] * 3,
        out_specs=(VMEM,) * 2,
        scratch_shapes=[columns],
        compiler_params=params(),
        name="third",
    )(peaks_of(peak, EVERY), state, raised)
    rows = lax.all_to_all(rows, "draw", 0, 0, tiled=True)
    peak = pl.pallas_call(
        join_kernel,
        out_shape=shape(mkt_count, 128),
        in_specs=[VMEM],
        out_specs=VMEM,
        compiler_params=params(),
        name="join",
    )(rows)
    jacobian, mean_util, norms = pl.pallas_call(
        final_kernel,
        out_shape=(shape(own, slots, slots), shape(markets, slots), shape(3)),
        in_specs=[VMEM] * 4,
        out_specs=(VMEM, VMEM, SMEM),
        scratch_shapes=[pltpu.VMEM((2, 128, draws), bf16), columns, pltpu.VMEM((own, 64, 128), f32)],
        compiler_params=params(),
        name="final",
    )(peaks_of(peak, "mkt"), state, rows, raised)
    return (mean_util, jacobian, norms)


def solution(mesh):
    return jax.shard_map(
        shards,
        mesh=mesh,
        in_specs=(P("mkt", None, None), P("mkt", None, "draw"), P(), P("mkt", None), P("mkt")),
        out_specs=(P("mkt", None), P(("mkt", "draw"), None, None), P()),
        check_vma=False,
    )
```

```python
import jax
import jax.numpy as jnp
from jax import lax
from jax.experimental import pallas as pl
from jax.experimental.pallas import tpu as pltpu
from jax.sharding import PartitionSpec as P

step_cap = 0.25
epsilon = 1e-06
LOG2E = 1.4426950408889634
VMEM = pl.BlockSpec(memory_space=pltpu.VMEM)
HBM = pl.BlockSpec(memory_space=pltpu.HBM)
SMEM = pl.BlockSpec(memory_space=pltpu.SMEM)
EVERY = ("mkt", "draw")


def pieces(value):
    high = value.astype(jnp.bfloat16).astype(jnp.float32)
    rest = value - high
    middle = rest.astype(jnp.bfloat16).astype(jnp.float32)
    return high, middle, rest - middle


def in_hbm(array):
    return pltpu.with_memory_space_constraint(array, pltpu.HBM)


def params(mebibytes=16):
    return pltpu.CompilerParams(vmem_limit_bytes=mebibytes << 20)


def column(value, slot, lanes=128):
    return jnp.broadcast_to(value[:, slot : slot + 1], (value.shape[0], lanes))


def fill(ref, value):
    tile = jnp.broadcast_to(value, (8, ref.shape[1]))
    for row in range(0, ref.shape[0], 8):
        ref[row : row + 8, :] = tile


def both_starts(copies):
    for copy in copies:
        copy.start()
    return copies


def sigma_levels(sigma_ref, depth, slots):
    level = lax.broadcasted_iota(jnp.int32, (depth, slots), 0)
    sigma = jnp.zeros((depth, slots), jnp.float32)
    for k in range(depth):
        sigma = jnp.where(level == k, sigma_ref[k], sigma)
    return sigma * LOG2E


def left_side(scaled):
    high, middle, low = pieces(scaled)
    left = jnp.concatenate([high, high, middle, high, low, middle], axis=0)
    return jnp.transpose(left).astype(jnp.bfloat16)


def raise_tastes(left, draws):
    high, middle, low = pieces(draws)
    right = jnp.concatenate([high, middle, high, low, high, middle], axis=0)
    return jnp.exp2(jnp.dot(left, right.astype(jnp.bfloat16), preferred_element_type=jnp.float32))


def usable_weights(state_ref, mean_util):
    return jnp.where(state_ref[1] > 0.0, jnp.exp(mean_util), 0.0)


def send_copies(sums_ref, sums):
    for d in range(sums_ref.shape[0]):
        sums_ref[d] = sums


def weight_columns(weights, columns_ref):
    for m in range(columns_ref.shape[0]):
        columns_ref[m] = column(weights, m)


def totals_over(columns_ref, raised_ref):
    markets, slots, draws = raised_ref.shape
    for m in range(markets):
        weight = columns_ref[m]
        total = jnp.zeros((slots, 128), jnp.float32)
        for g in range(0, draws, 128):
            raised = raised_ref[m, :, g : g + 128]
            below = 1.0 + jnp.sum(raised * weight, axis=0, keepdims=True)
            total = total + raised * (1.0 / below)
        columns_ref[m] = total


def packed_sums(totals_ref):
    markets, slots = totals_ref.shape[:2]
    lane = lax.broadcasted_iota(jnp.int32, (32, 128), 1)
    sums = jnp.zeros((32, 128), jnp.float32)
    upper = jnp.zeros((32, 128), jnp.float32)
    for m in range(markets):
        one = jnp.sum(totals_ref[m], axis=1, keepdims=True)
        rest = jnp.concatenate([one[32:slots], jnp.zeros((64 - slots, 1), jnp.float32)], axis=0)
        sums = jnp.where(lane == m, one[0:32], sums)
        upper = jnp.where(lane == m + 64, rest, upper)
    return jnp.where(lane < 64, sums, upper)


def start_kernel(counts_hbm, sigma_hbm, log_share_hbm, x_hbm, nu_hbm, state_ref, sums_ref, nu_ref, kept_ref, counts_ref, sigma_ref, rows_ref, log_share_ref, x_ref, left_ref, raised_ref, columns_ref, sems):
    markets, slots = log_share_hbm.shape
    depth = x_hbm.shape[1]
    chunk = markets // 4
    small = both_starts(
        [
            pltpu.make_async_copy(x_hbm, x_ref, sems.at[0]),
            pltpu.make_async_copy(sigma_hbm, sigma_ref, sems.at[1]),
            pltpu.make_async_copy(log_share_hbm, log_share_ref, sems.at[2]),
            pltpu.make_async_copy(counts_hbm, counts_ref, sems.at[3]),
        ]
    )
    large = both_starts(
        [
            pltpu.make_async_copy(nu_hbm.at[pl.ds(c * chunk, chunk)], nu_ref.at[pl.ds(c * chunk, chunk)], sems.at[4 + c])
            for c in range(4)
        ]
    )
    rows_ref[...] = jnp.zeros_like(rows_ref)
    for copy in small:
        copy.wait()
    sigma = sigma_levels(sigma_ref, depth, slots)
    for m in range(markets):
        left_ref[m] = left_side(x_ref[m] * sigma)
    base = lax.axis_index("draw") * kept_ref.shape[0]
    for m in range(kept_ref.shape[0]):
        kept_ref[m] = left_ref[base + m]
    rows_ref[0:markets, 0:slots] = log_share_ref[...]
    log_share = jnp.transpose(rows_ref[...])[0:slots, :]
    slot = lax.broadcasted_iota(jnp.int32, (slots, 128), 0)
    lane = lax.broadcasted_iota(jnp.int32, (8, 128), 1)
    count = jnp.zeros((8, 128), jnp.int32)
    for m in range(markets):
        count = jnp.where(lane == m, counts_ref[m], count)
    usable = slot < jnp.broadcast_to(count[0:1, :], (slots, 128))
    inside = jnp.sum(jnp.where(usable, jnp.exp(log_share), 0.0), axis=0, keepdims=True)
    mean_util = jnp.where(usable, log_share - jnp.log(1.0 - inside), 0.0)
    state_ref[0] = log_share
    state_ref[1] = jnp.where(usable, 1.0, 0.0)
    state_ref[2] = mean_util
    weight_columns(jnp.where(usable, jnp.exp(mean_util), 0.0), columns_ref)
    for copy in large:
        copy.wait()
    for m in range(markets):
        raised_ref[m] = raise_tastes(left_ref[m], nu_ref[m])
    totals_over(columns_ref, raised_ref)
    send_copies(sums_ref, packed_sums(columns_ref))


def stage_kernel(nu_ref, partner_ref, *sends):
    own = sends[0].shape[1]
    mine = lax.axis_index("draw")
    for k, send in enumerate(sends):
        first = (mine ^ (2 * (k + 1))) * own
        for m in range(own):
            send[0, m] = nu_ref[first + m]
            send[1, m] = partner_ref[first + m]


def keep_kernel(own, all_ref, kept_ref):
    slots = all_ref.shape[1]
    shift = 128 - lax.axis_index("draw") * own
    kept = lax.broadcasted_iota(jnp.int32, (slots, 8), 1) < own
    for p in range(3):
        kept_ref[p] = jnp.where(kept, pltpu.roll(all_ref[p], shift, axis=1)[:, 0:8], 0.0)


def change_kernel(inverse, own, sums_ref, all_ref, kept_ref, state_ref, peak_ref):
    mine = lax.axis_index("draw")
    total = sums_ref[0]
    for d in range(1, sums_ref.shape[0]):
        total = total + sums_ref[d]
    slots = all_ref.shape[1]
    sums = jnp.concatenate([total, pltpu.roll(total, 64, axis=1)[0 : slots - 32]], axis=0)
    usable = all_ref[1] > 0.0
    shares = sums * usable_weights(all_ref, all_ref[2]) * inverse
    change = jnp.where(usable, all_ref[0] - jnp.log(jnp.where(usable, shares, 1.0)), 0.0)
    fill(peak_ref, jnp.max(jnp.abs(change)))
    kept = lax.broadcasted_iota(jnp.int32, (slots, 8), 1) < own
    for p in range(3):
        state_ref[p] = kept_ref[p]
    state_ref[3] = jnp.where(kept, pltpu.roll(change, 128 - mine * own, axis=1)[:, 0:8], 0.0)
    state_ref[4] = jnp.zeros((slots, 8), jnp.float32)


def moved(turn, peaks_ref, state_ref):
    largest = jnp.max(peaks_ref[...])
    step = jnp.minimum(1.0, step_cap / (largest + epsilon))
    row = lax.broadcasted_iota(jnp.int32, state_ref.shape[1:], 0)
    return step, state_ref[2] + step * state_ref[3], jnp.where(row == turn, largest, state_ref[4])


def next_change(turn, peaks_ref, state_ref, out_ref, raised_ref, columns_ref):
    own, _, draws = raised_ref.shape
    _, mean_util, norms = moved(turn, peaks_ref, state_ref)
    usable = state_ref[1] > 0.0
    weights = jnp.where(usable, jnp.exp(mean_util), 0.0)
    weight_columns(weights, columns_ref)
    totals_over(columns_ref, raised_ref)
    lane = lax.broadcasted_iota(jnp.int32, weights.shape, 1)
    sums = jnp.ones(weights.shape, jnp.float32)
    for m in range(own):
        sums = jnp.where(lane == m, jnp.sum(columns_ref[m], axis=1, keepdims=True), sums)
    shares = sums * weights * (1.0 / draws)
    change = jnp.where(usable, state_ref[0] - jnp.log(jnp.where(usable, shares, 1.0)), 0.0)
    out_ref[0] = state_ref[0]
    out_ref[1] = state_ref[1]
    out_ref[2] = mean_util
    out_ref[3] = change
    out_ref[4] = norms
    return mean_util, change


def second_kernel(peaks_ref, state_ref, left_ref, nu_ref, partner_ref, *refs):
    received = refs[:3]
    raised_ref, out_ref, peak_ref, columns_ref = refs[3:]
    own = raised_ref.shape[0]
    base = lax.axis_index("draw") * own
    sources = [nu_ref.at[pl.ds(base, own)], partner_ref.at[pl.ds(base, own)]]
    for ref in received:
        sources += [ref.at[0], ref.at[1]]
    span = nu_ref.shape[2]
    for m in range(own):
        for s, source in enumerate(sources):
            raised_ref[m, :, s * span : (s + 1) * span] = raise_tastes(left_ref[m], source[m])
    _, change = next_change(0, peaks_ref, state_ref, out_ref, raised_ref, columns_ref)
    fill(peak_ref, jnp.max(jnp.abs(change)))


def as_rows(value):
    padded = jnp.concatenate([value, jnp.zeros((128 - value.shape[0], 8), jnp.float32)], axis=0)
    return jnp.transpose(padded)


def third_kernel(peaks_ref, state_ref, raised_ref, out_ref, rows_ref, columns_ref):
    mean_util, change = next_change(1, peaks_ref, state_ref, out_ref, raised_ref, columns_ref)
    send_copies(rows_ref, jnp.concatenate([as_rows(mean_util), as_rows(change)], axis=0))


def join_kernel(rows_ref, peak_ref):
    largest = jnp.abs(rows_ref[0, 8:16, :])
    for d in range(1, rows_ref.shape[0]):
        largest = jnp.maximum(largest, jnp.abs(rows_ref[d, 8:16, :]))
    fill(peak_ref, jnp.max(largest))


def final_kernel(peaks_ref, state_ref, rows_ref, raised_ref, jacobian_ref, mean_ref, norms_ref, both_ref, columns_ref, product_ref):
    own, slots, draws = raised_ref.shape
    step, mean_util, norms = moved(2, peaks_ref, state_ref)
    usable = state_ref[1]
    weight_columns(jnp.where(usable > 0.0, jnp.exp(mean_util), 0.0), columns_ref)
    usable_rows = as_rows(usable)
    for t in range(3):
        norms_ref[t] = jnp.max(norms[t : t + 1, :])
    for d in range(rows_ref.shape[0]):
        rows = rows_ref[d, 0:8, :] + step * rows_ref[d, 8:16, :]
        mean_ref[d * own : (d + 1) * own, :] = rows[0:own, 0:slots]
    padding = jnp.zeros((64 - slots, 128), jnp.float32)
    for m in range(own):
        weight = columns_ref[m]
        total = jnp.zeros((slots, 128), jnp.float32)
        buffer = m % 2
        for g in range(0, draws, 128):
            raised = raised_ref[m, :, g : g + 128] * weight
            chance = raised * (1.0 / (1.0 + jnp.sum(raised, axis=0, keepdims=True)))
            total = total + chance
            padded = jnp.concatenate([chance, padding], axis=0)
            high = padded.astype(jnp.bfloat16)
            low = (padded - high.astype(jnp.float32)).astype(jnp.bfloat16)
            both_ref[buffer, 0:64, g : g + 128] = high
            both_ref[buffer, 64:128, g : g + 128] = low
        columns_ref[m] = total
        product_ref[m] = lax.dot_general(
            both_ref[buffer],
            both_ref[buffer, 0:64, :],
            (((1,), (1,)), ((), ())),
            preferred_element_type=jnp.float32,
        )
    row = lax.broadcasted_iota(jnp.int32, (slots, slots), 0)
    col = lax.broadcasted_iota(jnp.int32, (slots, slots), 1)
    identity = jnp.where(row == col, 1.0, 0.0)
    for m in range(own):
        product = product_ref[m]
        crossed = product[64:128]
        cross = (product[0:64] + crossed + jnp.transpose(crossed))[0:slots, 0:slots]
        shares = jnp.sum(columns_ref[m], axis=1, keepdims=True)
        valid = column(usable, m, slots) > 0.0
        paired = valid & (usable_rows[m : m + 1, 0:slots] > 0.0)
        divisor = jnp.where(valid, shares, 1.0)
        jacobian_ref[m] = jnp.where(paired, identity - cross / divisor, 0.0)


def contract(x_char, nu_draws, coef_sigma, log_share, counts):
    markets, slots = log_share.shape
    depth, span = nu_draws.shape[1:]
    draw_count, mkt_count, every = (lax.axis_size(axis) for axis in ("draw", "mkt", EVERY))
    own = markets // draw_count
    draws = span * draw_count
    f32, bf16 = jnp.float32, jnp.bfloat16
    shape = lambda *sizes: jax.ShapeDtypeStruct(sizes, f32)
    state_shape = shape(5, slots, 8)
    columns = pltpu.VMEM((own, slots, 128), f32)

    def exchange(array, distance):
        return lax.ppermute(array, "draw", [(d, d ^ distance) for d in range(draw_count)])

    def peaks_of(peak, axis):
        count = peak.shape[0]
        return lax.all_to_all(peak.reshape(count, 1, 128), axis, 0, 0, tiled=True).reshape(count, 128)

    partner = exchange(nu_draws, 1)
    x_rows, sigma, nu_hbm = in_hbm(jnp.transpose(x_char, (0, 2, 1))), in_hbm(coef_sigma), in_hbm(nu_draws)
    all_state, sums, nu_near, left = pl.pallas_call(
        start_kernel,
        out_shape=(shape(3, slots, 128), shape(draw_count, 32, 128), shape(markets, depth, span), jax.ShapeDtypeStruct((own, slots, 6 * depth), bf16)),
        in_specs=[HBM] * 5,
        out_specs=(VMEM,) * 4,
        scratch_shapes=[
            pltpu.SMEM((markets,), jnp.int32),
            pltpu.SMEM((depth,), f32),
            pltpu.VMEM((128, 128), f32),
            pltpu.VMEM((markets, slots), f32),
            pltpu.VMEM((markets, depth, slots), f32),
            pltpu.VMEM((markets, slots, 6 * depth), bf16),
            pltpu.VMEM((markets, slots, span), f32),
            pltpu.VMEM((markets, slots, 128), f32),
            pltpu.SemaphoreType.DMA((8,)),
        ],
        compiler_params=params(),
        name="start",
    )(in_hbm(counts), sigma, in_hbm(log_share), x_rows, nu_hbm)
    sends = pl.pallas_call(
        stage_kernel,
        out_shape=(shape(2, own, depth, span),) * 3,
        in_specs=[VMEM] * 2,
        out_specs=(VMEM,) * 3,
        compiler_params=params(),
        name="stage",
    )(nu_near, partner)
    received = []
    for k, send in enumerate(sends):
        received.append(exchange(send, 2 * (k + 1)))
    sums = lax.all_to_all(sums, "draw", 0, 0, tiled=True)
    kept = pl.pallas_call(
        lambda *refs: keep_kernel(own, *refs),
        out_shape=shape(3, slots, 8),
        in_specs=[VMEM],
        out_specs=VMEM,
        compiler_params=params(),
        name="keep",
    )(all_state)
    state, peak = pl.pallas_call(
        lambda *refs: change_kernel(1.0 / draws, own, *refs),
        out_shape=(state_shape, shape(mkt_count, 128)),
        in_specs=[VMEM] * 3,
        out_specs=(VMEM,) * 2,
        compiler_params=params(),
        name="change",
    )(sums, all_state, kept)
    peaks = peaks_of(peak, "mkt")
    raised, state, peak = pl.pallas_call(
        second_kernel,
        out_shape=(shape(own, slots, draws), state_shape, shape(every, 128)),
        in_specs=[VMEM] * 8,
        out_specs=(VMEM,) * 3,
        scratch_shapes=[columns],
        compiler_params=params(),
        name="second",
    )(peaks, state, left, nu_near, partner, *received)
    state, rows = pl.pallas_call(
        third_kernel,
        out_shape=(state_shape, shape(draw_count, 16, 128)),
        in_specs=[VMEM] * 3,
        out_specs=(VMEM,) * 2,
        scratch_shapes=[columns],
        compiler_params=params(),
        name="third",
    )(peaks_of(peak, EVERY), state, raised)
    rows = lax.all_to_all(rows, "draw", 0, 0, tiled=True)
    peak = pl.pallas_call(
        join_kernel,
        out_shape=shape(mkt_count, 128),
        in_specs=[VMEM],
        out_specs=VMEM,
        compiler_params=params(),
        name="join",
    )(rows)
    jacobian, mean_util, norms = pl.pallas_call(
        final_kernel,
        out_shape=(shape(own, slots, slots), shape(markets, slots), shape(3)),
        in_specs=[VMEM] * 4,
        out_specs=(VMEM, VMEM, SMEM),
        scratch_shapes=[pltpu.VMEM((2, 128, draws), bf16), columns, pltpu.VMEM((own, 128, 64), f32)],
        compiler_params=params(),
        name="final",
    )(peaks_of(peak, "mkt"), state, rows, raised)
    return (mean_util, jacobian, norms)


def solution(mesh):
    return jax.shard_map(
        contract,
        mesh=mesh,
        in_specs=(P("mkt", None, None), P("mkt", None, "draw"), P(), P("mkt", None), P("mkt")),
        out_specs=(P("mkt", None), P(("mkt", "draw"), None, None), P()),
        check_vma=False,
    )
```

```python
import jax
import jax.numpy as jnp
from jax import lax
from jax.experimental import pallas as pl
from jax.experimental.pallas import tpu as pltpu
from jax.sharding import PartitionSpec as P

step_cap = 0.25
epsilon = 1e-06
LOG2E = 1.4426950408889634
VMEM = pl.BlockSpec(memory_space=pltpu.VMEM)
HBM = pl.BlockSpec(memory_space=pltpu.HBM)
SMEM = pl.BlockSpec(memory_space=pltpu.SMEM)
EVERY = ("mkt", "draw")


def pieces(value):
    high = value.astype(jnp.bfloat16).astype(jnp.float32)
    rest = value - high
    middle = rest.astype(jnp.bfloat16).astype(jnp.float32)
    return high, middle, rest - middle


def in_hbm(array):
    return pltpu.with_memory_space_constraint(array, pltpu.HBM)


def params(mebibytes=16):
    return pltpu.CompilerParams(vmem_limit_bytes=mebibytes << 20)


def column(value, slot, lanes=128):
    return jnp.broadcast_to(value[:, slot : slot + 1], (value.shape[0], lanes))


def fill(ref, value):
    tile = jnp.broadcast_to(value, (8, ref.shape[1]))
    for row in range(0, ref.shape[0], 8):
        ref[row : row + 8, :] = tile


def both_starts(copies):
    for copy in copies:
        copy.start()
    return copies


def sigma_levels(sigma_ref, depth, slots):
    level = lax.broadcasted_iota(jnp.int32, (depth, slots), 0)
    sigma = jnp.zeros((depth, slots), jnp.float32)
    for k in range(depth):
        sigma = jnp.where(level == k, sigma_ref[k], sigma)
    return sigma * LOG2E


def left_side(scaled):
    high, middle, low = pieces(scaled)
    left = jnp.concatenate([high, high, middle, high, low, middle], axis=0)
    return jnp.transpose(left.astype(jnp.bfloat16))


def raise_tastes(left, draws):
    high, middle, low = pieces(draws)
    right = jnp.concatenate([high, middle, high, low, high, middle], axis=0)
    return jnp.exp2(jnp.dot(left, right.astype(jnp.bfloat16), preferred_element_type=jnp.float32))


def usable_weights(state_ref, mean_util):
    return jnp.where(state_ref[1] > 0.0, jnp.exp(mean_util), 0.0)


def send_copies(sums_ref, sums):
    for d in range(sums_ref.shape[0]):
        sums_ref[d] = sums


def weight_columns(weights, columns_ref):
    for m in range(columns_ref.shape[0]):
        columns_ref[m] = column(weights, m)


def eights(markets, draws):
    units = [(m, g) for m in markets for g in range(0, draws, 128)]
    return [units[u : u + 8] for u in range(0, len(units), 8)]


def inverse_rows(units, slot, columns_ref, raised_ref, parts_ref, inverse_ref):
    slots = raised_ref.shape[1]
    for u, (m, g) in enumerate(units):
        part = raised_ref[m, 0:8, g : g + 128] * columns_ref[m, 0:8, :]
        for j in range(8, slots, 8):
            part = part + raised_ref[m, j : j + 8, g : g + 128] * columns_ref[m, j : j + 8, :]
        parts_ref[slot, 8 * u : 8 * u + 8, :] = part
    below = parts_ref[slot, pl.ds(0, 8, stride=8), :] + 1.0
    for j in range(1, 8):
        below = below + parts_ref[slot, pl.ds(j, 8, stride=8), :]
    inverse_ref[slot] = 1.0 / below


def totals_over(columns_ref, raised_ref, parts_ref, inverse_ref, totals_ref):
    markets, slots, draws = raised_ref.shape
    for b, units in enumerate(eights(range(markets), draws)):
        slot = b % parts_ref.shape[0]
        inverse_rows(units, slot, columns_ref, raised_ref, parts_ref, inverse_ref)
        for m in sorted(set(m for m, _ in units)):
            total = jnp.zeros((slots, 128), jnp.float32)
            for u, (other, g) in enumerate(units):
                if other == m:
                    total = total + raised_ref[m, :, g : g + 128] * inverse_ref[slot, u : u + 1, :]
            if any(g == 0 for other, g in units if other == m):
                totals_ref[m] = total
            else:
                totals_ref[m] += total


def packed_sums(totals_ref):
    markets, slots = totals_ref.shape[:2]
    lane = lax.broadcasted_iota(jnp.int32, (32, 128), 1)
    sums = jnp.zeros((32, 128), jnp.float32)
    upper = jnp.zeros((32, 128), jnp.float32)
    for m in range(markets):
        one = jnp.sum(totals_ref[m], axis=1, keepdims=True)
        rest = jnp.concatenate([one[32:slots], jnp.zeros((64 - slots, 1), jnp.float32)], axis=0)
        sums = jnp.where(lane == m, one[0:32], sums)
        upper = jnp.where(lane == m + 64, rest, upper)
    return jnp.where(lane < 64, sums, upper)


def start_kernel(counts_hbm, sigma_hbm, log_share_hbm, x_hbm, nu_hbm, state_ref, sums_ref, nu_ref, kept_ref, counts_ref, sigma_ref, rows_ref, log_share_ref, x_ref, left_ref, raised_ref, columns_ref, totals_ref, parts_ref, inverse_ref, sems):
    markets, slots = log_share_hbm.shape
    depth = x_hbm.shape[1]
    chunk = markets // 4
    small = both_starts(
        [
            pltpu.make_async_copy(x_hbm, x_ref, sems.at[0]),
            pltpu.make_async_copy(sigma_hbm, sigma_ref, sems.at[1]),
            pltpu.make_async_copy(log_share_hbm, log_share_ref, sems.at[2]),
            pltpu.make_async_copy(counts_hbm, counts_ref, sems.at[3]),
        ]
    )
    large = both_starts(
        [
            pltpu.make_async_copy(nu_hbm.at[pl.ds(c * chunk, chunk)], nu_ref.at[pl.ds(c * chunk, chunk)], sems.at[4 + c])
            for c in range(4)
        ]
    )
    rows_ref[...] = jnp.zeros_like(rows_ref)
    for copy in small:
        copy.wait()
    sigma = sigma_levels(sigma_ref, depth, slots)
    for m in range(markets):
        left_ref[m] = left_side(x_ref[m] * sigma)
    base = lax.axis_index("draw") * kept_ref.shape[0]
    for m in range(kept_ref.shape[0]):
        kept_ref[m] = left_ref[base + m]
    rows_ref[0:markets, 0:slots] = log_share_ref[...]
    log_share = jnp.transpose(rows_ref[...])[0:slots, :]
    slot = lax.broadcasted_iota(jnp.int32, (slots, 128), 0)
    lane = lax.broadcasted_iota(jnp.int32, (8, 128), 1)
    count = jnp.zeros((8, 128), jnp.int32)
    for m in range(markets):
        count = jnp.where(lane == m, counts_ref[m], count)
    usable = slot < jnp.broadcast_to(count[0:1, :], (slots, 128))
    inside = jnp.sum(jnp.where(usable, jnp.exp(log_share), 0.0), axis=0, keepdims=True)
    mean_util = jnp.where(usable, log_share - jnp.log(1.0 - inside), 0.0)
    state_ref[0] = log_share
    state_ref[1] = jnp.where(usable, 1.0, 0.0)
    state_ref[2] = mean_util
    weight_columns(jnp.where(usable, jnp.exp(mean_util), 0.0), columns_ref)
    for copy in large:
        copy.wait()
    for m in range(markets):
        raised_ref[m] = raise_tastes(left_ref[m], nu_ref[m])
    totals_over(columns_ref, raised_ref, parts_ref, inverse_ref, totals_ref)
    send_copies(sums_ref, packed_sums(totals_ref))


def stage_kernel(nu_ref, partner_ref, *sends):
    own = sends[0].shape[1]
    mine = lax.axis_index("draw")
    for k, send in enumerate(sends):
        first = (mine ^ (2 * (k + 1))) * own
        for m in range(own):
            send[0, m] = nu_ref[first + m]
            send[1, m] = partner_ref[first + m]


def keep_kernel(own, all_ref, kept_ref):
    slots = all_ref.shape[1]
    shift = 128 - lax.axis_index("draw") * own
    kept = lax.broadcasted_iota(jnp.int32, (slots, 8), 1) < own
    for p in range(3):
        kept_ref[p] = jnp.where(kept, pltpu.roll(all_ref[p], shift, axis=1)[:, 0:8], 0.0)


def change_kernel(inverse, own, sums_ref, all_ref, kept_ref, state_ref, peak_ref):
    mine = lax.axis_index("draw")
    total = sums_ref[0]
    for d in range(1, sums_ref.shape[0]):
        total = total + sums_ref[d]
    slots = all_ref.shape[1]
    sums = jnp.concatenate([total, pltpu.roll(total, 64, axis=1)[0 : slots - 32]], axis=0)
    usable = all_ref[1] > 0.0
    shares = sums * usable_weights(all_ref, all_ref[2]) * inverse
    change = jnp.where(usable, all_ref[0] - jnp.log(jnp.where(usable, shares, 1.0)), 0.0)
    fill(peak_ref, jnp.max(jnp.abs(change)))
    kept = lax.broadcasted_iota(jnp.int32, (slots, 8), 1) < own
    for p in range(3):
        state_ref[p] = kept_ref[p]
    state_ref[3] = jnp.where(kept, pltpu.roll(change, 128 - mine * own, axis=1)[:, 0:8], 0.0)
    state_ref[4] = jnp.zeros((slots, 8), jnp.float32)


def moved(turn, peaks_ref, state_ref):
    largest = jnp.max(peaks_ref[...])
    step = jnp.minimum(1.0, step_cap / (largest + epsilon))
    row = lax.broadcasted_iota(jnp.int32, state_ref.shape[1:], 0)
    return step, state_ref[2] + step * state_ref[3], jnp.where(row == turn, largest, state_ref[4])


def next_change(turn, peaks_ref, state_ref, out_ref, raised_ref, columns_ref, totals_ref, *eight):
    own, _, draws = raised_ref.shape
    _, mean_util, norms = moved(turn, peaks_ref, state_ref)
    usable = state_ref[1] > 0.0
    weights = jnp.where(usable, jnp.exp(mean_util), 0.0)
    weight_columns(weights, columns_ref)
    totals_over(columns_ref, raised_ref, *eight, totals_ref)
    lane = lax.broadcasted_iota(jnp.int32, weights.shape, 1)
    sums = jnp.ones(weights.shape, jnp.float32)
    for m in range(own):
        sums = jnp.where(lane == m, jnp.sum(totals_ref[m], axis=1, keepdims=True), sums)
    shares = sums * weights * (1.0 / draws)
    change = jnp.where(usable, state_ref[0] - jnp.log(jnp.where(usable, shares, 1.0)), 0.0)
    out_ref[0] = state_ref[0]
    out_ref[1] = state_ref[1]
    out_ref[2] = mean_util
    out_ref[3] = change
    out_ref[4] = norms
    return mean_util, change


def second_kernel(peaks_ref, state_ref, left_ref, nu_ref, partner_ref, *refs):
    received = refs[:3]
    raised_ref, out_ref, peak_ref, *scratch = refs[3:]
    own = raised_ref.shape[0]
    base = lax.axis_index("draw") * own
    sources = [nu_ref.at[pl.ds(base, own)], partner_ref.at[pl.ds(base, own)]]
    for ref in received:
        sources += [ref.at[0], ref.at[1]]
    span = nu_ref.shape[2]
    for m in range(own):
        for s, source in enumerate(sources):
            raised_ref[m, :, s * span : (s + 1) * span] = raise_tastes(left_ref[m], source[m])
    _, change = next_change(0, peaks_ref, state_ref, out_ref, raised_ref, *scratch)
    fill(peak_ref, jnp.max(jnp.abs(change)))


def as_rows(value):
    padded = jnp.concatenate([value, jnp.zeros((128 - value.shape[0], 8), jnp.float32)], axis=0)
    return jnp.transpose(padded)


def third_kernel(peaks_ref, state_ref, raised_ref, out_ref, rows_ref, *scratch):
    mean_util, change = next_change(1, peaks_ref, state_ref, out_ref, raised_ref, *scratch)
    send_copies(rows_ref, jnp.concatenate([as_rows(mean_util), as_rows(change)], axis=0))


def join_kernel(rows_ref, peak_ref):
    largest = jnp.abs(rows_ref[0, 8:16, :])
    for d in range(1, rows_ref.shape[0]):
        largest = jnp.maximum(largest, jnp.abs(rows_ref[d, 8:16, :]))
    fill(peak_ref, jnp.max(largest))


def final_kernel(peaks_ref, state_ref, rows_ref, raised_ref, jacobian_ref, mean_ref, norms_ref, even_ref, odd_ref, columns_ref, product_ref, parts_ref, inverse_ref):
    own, slots, draws = raised_ref.shape
    step, mean_util, norms = moved(2, peaks_ref, state_ref)
    usable = state_ref[1]
    weight_columns(jnp.where(usable > 0.0, jnp.exp(mean_util), 0.0), columns_ref)
    usable_rows = as_rows(usable)
    for t in range(3):
        norms_ref[t] = jnp.max(norms[t : t + 1, :])
    for d in range(rows_ref.shape[0]):
        rows = rows_ref[d, 0:8, :] + step * rows_ref[d, 8:16, :]
        mean_ref[d * own : (d + 1) * own, :] = rows[0:own, 0:slots]
    below = lax.broadcasted_iota(jnp.int32, (64 - slots, 128), 0)
    padding = jnp.where(below == 0, 1.0, 0.0)

    def chances(m, both_ref):
        for b, units in enumerate(eights([m], draws)):
            inverse_rows(units, b, columns_ref, raised_ref, parts_ref, inverse_ref)
            for u, (_, g) in enumerate(units):
                chance = raised_ref[m, :, g : g + 128] * columns_ref[m] * inverse_ref[b, u : u + 1, :]
                padded = jnp.concatenate([chance, padding], axis=0)
                high = padded.astype(jnp.bfloat16)
                both_ref[0:64, g : g + 128] = high
                both_ref[64:128, g : g + 128] = (padded - high.astype(jnp.float32)).astype(jnp.bfloat16)

    def products(m, both_ref):
        product_ref[m] = lax.dot_general(
            both_ref[...], both_ref[0:64, :], (((1,), (1,)), ((), ())), preferred_element_type=jnp.float32
        )

    def pair(p, carry):
        products(2 * p, even_ref)
        chances(2 * p + 1, odd_ref)
        products(2 * p + 1, odd_ref)
        chances(2 * p + 2, even_ref)
        return carry

    chances(0, even_ref)
    lax.fori_loop(0, own // 2 - 1, pair, 0)
    products(own - 2, even_ref)
    chances(own - 1, odd_ref)
    products(own - 1, odd_ref)
    row = lax.broadcasted_iota(jnp.int32, (slots, slots), 0)
    col = lax.broadcasted_iota(jnp.int32, (slots, slots), 1)
    identity = jnp.where(row == col, 1.0, 0.0)
    for m in range(own):
        product = product_ref[m]
        crossed = product[64:128]
        cross = (product[0:64] + crossed + jnp.transpose(crossed))[0:slots, 0:slots]
        shares = (product[0:64] + crossed)[0:slots, slots : slots + 1]
        valid = column(usable, m, slots) > 0.0
        paired = valid & (usable_rows[m : m + 1, 0:slots] > 0.0)
        divisor = jnp.where(valid, shares, 1.0)
        jacobian_ref[m] = jnp.where(paired, identity - cross / divisor, 0.0)


def contract(x_char, nu_draws, coef_sigma, log_share, counts):
    markets, slots = log_share.shape
    depth, span = nu_draws.shape[1:]
    draw_count, mkt_count, every = (lax.axis_size(axis) for axis in ("draw", "mkt", EVERY))
    own = markets // draw_count
    draws = span * draw_count
    f32, bf16 = jnp.float32, jnp.bfloat16
    shape = lambda *sizes: jax.ShapeDtypeStruct(sizes, f32)
    state_shape = shape(5, slots, 8)
    columns = pltpu.VMEM((own, slots, 128), f32)
    eight = [pltpu.VMEM((4, 64, 128), f32), pltpu.VMEM((4, 8, 128), f32)]

    def exchange(array, distance):
        return lax.ppermute(array, "draw", [(d, d ^ distance) for d in range(draw_count)])

    def peaks_of(peak, axis):
        count = peak.shape[0]
        return lax.all_to_all(peak.reshape(count, 1, 128), axis, 0, 0, tiled=True).reshape(count, 128)

    partner = exchange(nu_draws, 1)
    x_rows, sigma, nu_hbm = in_hbm(jnp.transpose(x_char, (0, 2, 1))), in_hbm(coef_sigma), in_hbm(nu_draws)
    all_state, sums, nu_near, left = pl.pallas_call(
        start_kernel,
        out_shape=(shape(3, slots, 128), shape(draw_count, 32, 128), shape(markets, depth, span), jax.ShapeDtypeStruct((own, slots, 6 * depth), bf16)),
        in_specs=[HBM] * 5,
        out_specs=(VMEM,) * 4,
        scratch_shapes=[
            pltpu.SMEM((markets,), jnp.int32),
            pltpu.SMEM((depth,), f32),
            pltpu.VMEM((128, 128), f32),
            pltpu.VMEM((markets, slots), f32),
            pltpu.VMEM((markets, depth, slots), f32),
            pltpu.VMEM((markets, slots, 6 * depth), bf16),
            pltpu.VMEM((markets, slots, span), f32),
            pltpu.VMEM((markets, slots, 128), f32),
            pltpu.VMEM((markets, slots, 128), f32),
            *eight,
            pltpu.SemaphoreType.DMA((8,)),
        ],
        compiler_params=params(),
        name="start",
    )(in_hbm(counts), sigma, in_hbm(log_share), x_rows, nu_hbm)
    sends = pl.pallas_call(
        stage_kernel,
        out_shape=(shape(2, own, depth, span),) * 3,
        in_specs=[VMEM] * 2,
        out_specs=(VMEM,) * 3,
        compiler_params=params(),
        name="stage",
    )(nu_near, partner)
    received = []
    for k, send in enumerate(sends):
        received.append(exchange(send, 2 * (k + 1)))
    sums = lax.all_to_all(sums, "draw", 0, 0, tiled=True)
    kept = pl.pallas_call(
        lambda *refs: keep_kernel(own, *refs),
        out_shape=shape(3, slots, 8),
        in_specs=[VMEM],
        out_specs=VMEM,
        compiler_params=params(),
        name="keep",
    )(all_state)
    state, peak = pl.pallas_call(
        lambda *refs: change_kernel(1.0 / draws, own, *refs),
        out_shape=(state_shape, shape(mkt_count, 128)),
        in_specs=[VMEM] * 3,
        out_specs=(VMEM,) * 2,
        compiler_params=params(),
        name="change",
    )(sums, all_state, kept)
    peaks = peaks_of(peak, "mkt")
    raised, state, peak = pl.pallas_call(
        second_kernel,
        out_shape=(shape(own, slots, draws), state_shape, shape(every, 128)),
        in_specs=[VMEM] * 8,
        out_specs=(VMEM,) * 3,
        scratch_shapes=[columns, columns, *eight],
        compiler_params=params(),
        name="second",
    )(peaks, state, left, nu_near, partner, *received)
    state, rows = pl.pallas_call(
        third_kernel,
        out_shape=(state_shape, shape(draw_count, 16, 128)),
        in_specs=[VMEM] * 3,
        out_specs=(VMEM,) * 2,
        scratch_shapes=[columns, columns, *eight],
        compiler_params=params(),
        name="third",
    )(peaks_of(peak, EVERY), state, raised)
    rows = lax.all_to_all(rows, "draw", 0, 0, tiled=True)
    peak = pl.pallas_call(
        join_kernel,
        out_shape=shape(mkt_count, 128),
        in_specs=[VMEM],
        out_specs=VMEM,
        compiler_params=params(),
        name="join",
    )(rows)
    jacobian, mean_util, norms = pl.pallas_call(
        final_kernel,
        out_shape=(shape(own, slots, slots), shape(markets, slots), shape(3)),
        in_specs=[VMEM] * 4,
        out_specs=(VMEM, VMEM, SMEM),
        scratch_shapes=[pltpu.VMEM((128, draws), bf16)] * 2 + [columns, pltpu.VMEM((own, 128, 64), f32), *eight],
        compiler_params=params(),
        name="final",
    )(peaks_of(peak, "mkt"), state, rows, raised)
    return (mean_util, jacobian, norms)


def solution(mesh):
    return jax.shard_map(
        contract,
        mesh=mesh,
        in_specs=(P("mkt", None, None), P("mkt", None, "draw"), P(), P("mkt", None), P("mkt")),
        out_specs=(P("mkt", None), P(("mkt", "draw"), None, None), P()),
        check_vma=False,
    )
```

```python
import jax
import jax.numpy as jnp
from jax import lax
from jax.experimental import pallas as pl
from jax.experimental.pallas import tpu as pltpu
from jax.sharding import PartitionSpec as P

step_cap = 0.25
epsilon = 1e-06
LOG2E = 1.4426950408889634
VMEM = pl.BlockSpec(memory_space=pltpu.VMEM)
HBM = pl.BlockSpec(memory_space=pltpu.HBM)
SMEM = pl.BlockSpec(memory_space=pltpu.SMEM)
EVERY = ("mkt", "draw")


def pieces(value):
    high = value.astype(jnp.bfloat16).astype(jnp.float32)
    rest = value - high
    middle = rest.astype(jnp.bfloat16).astype(jnp.float32)
    return high, middle, rest - middle


def in_hbm(array):
    return pltpu.with_memory_space_constraint(array, pltpu.HBM)


def params(mebibytes=16):
    return pltpu.CompilerParams(vmem_limit_bytes=mebibytes << 20)


def column(value, slot, lanes=128):
    return jnp.broadcast_to(value[:, slot : slot + 1], (value.shape[0], lanes))


def fill(ref, value):
    tile = jnp.broadcast_to(value, (8, ref.shape[1]))
    for row in range(0, ref.shape[0], 8):
        ref[row : row + 8, :] = tile


def both_starts(copies):
    for copy in copies:
        copy.start()
    return copies


def sigma_levels(sigma_ref, depth, slots):
    level = lax.broadcasted_iota(jnp.int32, (depth, slots), 0)
    sigma = jnp.zeros((depth, slots), jnp.float32)
    for k in range(depth):
        sigma = jnp.where(level == k, sigma_ref[k], sigma)
    return sigma * LOG2E


def left_side(scaled):
    high, middle, low = pieces(scaled)
    left = jnp.concatenate([high, high, middle, high, low, middle], axis=0)
    return jnp.transpose(left.astype(jnp.bfloat16))


def raise_tastes(left, draws):
    high, middle, low = pieces(draws)
    right = jnp.concatenate([high, middle, high, low, high, middle], axis=0)
    return jnp.exp2(jnp.dot(left, right.astype(jnp.bfloat16), preferred_element_type=jnp.float32))


def usable_weights(state_ref, mean_util):
    return jnp.where(state_ref[1] > 0.0, jnp.exp(mean_util), 0.0)


def send_copies(sums_ref, sums):
    for d in range(sums_ref.shape[0]):
        sums_ref[d] = sums


def weight_columns(weights, columns_ref):
    for m in range(columns_ref.shape[0]):
        columns_ref[m] = column(weights, m)


def inverse_rows(columns_ref, raised_ref, parts_ref, inverse_ref):
    markets, slots, draws = raised_ref.shape
    units = [(m, g) for m in range(markets) for g in range(0, draws, 128)]
    for u, (m, g) in enumerate(units):
        part = raised_ref[m, 0:8, g : g + 128] * columns_ref[m, 0:8, :]
        for j in range(8, slots, 8):
            part = part + raised_ref[m, j : j + 8, g : g + 128] * columns_ref[m, j : j + 8, :]
        parts_ref[8 * u : 8 * u + 8, :] = part
    for u in range(0, len(units), 8):
        below = parts_ref[pl.ds(8 * u, 8, stride=8), :] + 1.0
        for j in range(1, 8):
            below = below + parts_ref[pl.ds(8 * u + j, 8, stride=8), :]
        inverse_ref[u : u + 8, :] = 1.0 / below


def totals_over(columns_ref, raised_ref, parts_ref, inverse_ref, totals_ref):
    markets, slots, draws = raised_ref.shape
    inverse_rows(columns_ref, raised_ref, parts_ref, inverse_ref)
    groups = draws // 128
    for m in range(markets):
        total = jnp.zeros((slots, 128), jnp.float32)
        for g in range(groups):
            u = m * groups + g
            total = total + raised_ref[m, :, 128 * g : 128 * g + 128] * inverse_ref[u : u + 1, :]
        totals_ref[m] = total


def send_lane_sums(sums_ref, totals_ref):
    markets, slots = totals_ref.shape[:2]
    lane = lax.broadcasted_iota(jnp.int32, (slots, 128), 1)
    ones = jnp.ones((256, 128), jnp.bfloat16)
    sums = jnp.zeros((slots, 128), jnp.float32)
    for m in range(markets):
        total = totals_ref[m]
        high = total.astype(jnp.bfloat16)
        low = (total - high.astype(jnp.float32)).astype(jnp.bfloat16)
        both = jnp.concatenate([high, low], axis=1)
        sums = jnp.where(lane == m, jnp.dot(both, ones, preferred_element_type=jnp.float32), sums)
    rest = jnp.concatenate([sums[32:slots], jnp.zeros((64 - slots, 128), jnp.float32)], axis=0)
    send_copies(sums_ref, jnp.where(lane[0:32] < 64, sums[0:32], pltpu.roll(rest, 64, axis=1)))


def start_kernel(counts_hbm, sigma_hbm, log_share_hbm, x_hbm, nu_hbm, state_ref, sums_ref, nu_ref, kept_ref, counts_ref, sigma_ref, rows_ref, log_share_ref, x_ref, left_ref, raised_ref, columns_ref, totals_ref, parts_ref, inverse_ref, sems):
    markets, slots = log_share_hbm.shape
    depth = x_hbm.shape[1]
    chunk = markets // 4
    small = both_starts(
        [
            pltpu.make_async_copy(x_hbm, x_ref, sems.at[0]),
            pltpu.make_async_copy(sigma_hbm, sigma_ref, sems.at[1]),
            pltpu.make_async_copy(log_share_hbm, log_share_ref, sems.at[2]),
            pltpu.make_async_copy(counts_hbm, counts_ref, sems.at[3]),
        ]
    )
    large = both_starts(
        [
            pltpu.make_async_copy(nu_hbm.at[pl.ds(c * chunk, chunk)], nu_ref.at[pl.ds(c * chunk, chunk)], sems.at[4 + c])
            for c in range(4)
        ]
    )
    rows_ref[...] = jnp.zeros_like(rows_ref)
    for copy in small:
        copy.wait()
    sigma = sigma_levels(sigma_ref, depth, slots)
    for m in range(markets):
        left_ref[m] = left_side(x_ref[m] * sigma)
    base = lax.axis_index("draw") * kept_ref.shape[0]
    for m in range(kept_ref.shape[0]):
        kept_ref[m] = left_ref[base + m]
    rows_ref[0:markets, 0:slots] = log_share_ref[...]
    log_share = jnp.transpose(rows_ref[...])[0:slots, :]
    slot = lax.broadcasted_iota(jnp.int32, (slots, 128), 0)
    lane = lax.broadcasted_iota(jnp.int32, (8, 128), 1)
    count = jnp.zeros((8, 128), jnp.int32)
    for m in range(markets):
        count = jnp.where(lane == m, counts_ref[m], count)
    usable = slot < jnp.broadcast_to(count[0:1, :], (slots, 128))
    inside = jnp.sum(jnp.where(usable, jnp.exp(log_share), 0.0), axis=0, keepdims=True)
    mean_util = jnp.where(usable, log_share - jnp.log(1.0 - inside), 0.0)
    state_ref[0] = log_share
    state_ref[1] = jnp.where(usable, 1.0, 0.0)
    state_ref[2] = mean_util
    weight_columns(jnp.where(usable, jnp.exp(mean_util), 0.0), columns_ref)
    for copy in large:
        copy.wait()
    for m in range(markets):
        raised_ref[m] = raise_tastes(left_ref[m], nu_ref[m])
    totals_over(columns_ref, raised_ref, parts_ref, inverse_ref, totals_ref)
    send_lane_sums(sums_ref, totals_ref)


def stage_kernel(nu_ref, partner_ref, *sends):
    own = sends[0].shape[1]
    mine = lax.axis_index("draw")
    for k, send in enumerate(sends):
        first = (mine ^ (2 * (k + 1))) * own
        for m in range(own):
            send[0, m] = nu_ref[first + m]
            send[1, m] = partner_ref[first + m]


def keep_kernel(own, all_ref, kept_ref):
    slots = all_ref.shape[1]
    shift = 128 - lax.axis_index("draw") * own
    kept = lax.broadcasted_iota(jnp.int32, (slots, 8), 1) < own
    for p in range(3):
        kept_ref[p] = jnp.where(kept, pltpu.roll(all_ref[p], shift, axis=1)[:, 0:8], 0.0)


def change_kernel(inverse, own, sums_ref, all_ref, kept_ref, state_ref, peak_ref):
    mine = lax.axis_index("draw")
    total = sums_ref[0]
    for d in range(1, sums_ref.shape[0]):
        total = total + sums_ref[d]
    slots = all_ref.shape[1]
    sums = jnp.concatenate([total, pltpu.roll(total, 64, axis=1)[0 : slots - 32]], axis=0)
    usable = all_ref[1] > 0.0
    shares = sums * usable_weights(all_ref, all_ref[2]) * inverse
    change = jnp.where(usable, all_ref[0] - jnp.log(jnp.where(usable, shares, 1.0)), 0.0)
    fill(peak_ref, jnp.max(jnp.abs(change)))
    kept = lax.broadcasted_iota(jnp.int32, (slots, 8), 1) < own
    for p in range(3):
        state_ref[p] = kept_ref[p]
    state_ref[3] = jnp.where(kept, pltpu.roll(change, 128 - mine * own, axis=1)[:, 0:8], 0.0)
    state_ref[4] = jnp.zeros((slots, 8), jnp.float32)


def moved(turn, peaks_ref, state_ref):
    largest = jnp.max(peaks_ref[...])
    step = jnp.minimum(1.0, step_cap / (largest + epsilon))
    row = lax.broadcasted_iota(jnp.int32, state_ref.shape[1:], 0)
    return step, state_ref[2] + step * state_ref[3], jnp.where(row == turn, largest, state_ref[4])


def next_change(turn, peaks_ref, state_ref, out_ref, raised_ref, columns_ref, totals_ref, *eight):
    own, _, draws = raised_ref.shape
    _, mean_util, norms = moved(turn, peaks_ref, state_ref)
    usable = state_ref[1] > 0.0
    weights = jnp.where(usable, jnp.exp(mean_util), 0.0)
    weight_columns(weights, columns_ref)
    totals_over(columns_ref, raised_ref, *eight, totals_ref)
    lane = lax.broadcasted_iota(jnp.int32, weights.shape, 1)
    sums = jnp.ones(weights.shape, jnp.float32)
    for m in range(own):
        sums = jnp.where(lane == m, jnp.sum(totals_ref[m], axis=1, keepdims=True), sums)
    shares = sums * weights * (1.0 / draws)
    change = jnp.where(usable, state_ref[0] - jnp.log(jnp.where(usable, shares, 1.0)), 0.0)
    out_ref[0] = state_ref[0]
    out_ref[1] = state_ref[1]
    out_ref[2] = mean_util
    out_ref[3] = change
    out_ref[4] = norms
    return mean_util, change


def second_kernel(peaks_ref, state_ref, left_ref, nu_ref, partner_ref, *refs):
    received = refs[:3]
    raised_ref, out_ref, peak_ref, *scratch = refs[3:]
    own = raised_ref.shape[0]
    base = lax.axis_index("draw") * own
    sources = [nu_ref.at[pl.ds(base, own)], partner_ref.at[pl.ds(base, own)]]
    for ref in received:
        sources += [ref.at[0], ref.at[1]]
    span = nu_ref.shape[2]
    for m in range(own):
        for s, source in enumerate(sources):
            raised_ref[m, :, s * span : (s + 1) * span] = raise_tastes(left_ref[m], source[m])
    _, change = next_change(0, peaks_ref, state_ref, out_ref, raised_ref, *scratch)
    fill(peak_ref, jnp.max(jnp.abs(change)))


def as_rows(value):
    padded = jnp.concatenate([value, jnp.zeros((128 - value.shape[0], 8), jnp.float32)], axis=0)
    return jnp.transpose(padded)


def third_kernel(peaks_ref, state_ref, raised_ref, out_ref, rows_ref, *scratch):
    mean_util, change = next_change(1, peaks_ref, state_ref, out_ref, raised_ref, *scratch)
    send_copies(rows_ref, jnp.concatenate([as_rows(mean_util), as_rows(change)], axis=0))


def join_kernel(rows_ref, peak_ref):
    largest = jnp.abs(rows_ref[0, 8:16, :])
    for d in range(1, rows_ref.shape[0]):
        largest = jnp.maximum(largest, jnp.abs(rows_ref[d, 8:16, :]))
    fill(peak_ref, jnp.max(largest))


def final_kernel(peaks_ref, state_ref, rows_ref, raised_ref, jacobian_ref, mean_ref, norms_ref, even_ref, odd_ref, columns_ref, product_ref, parts_ref, inverse_ref):
    own, slots, draws = raised_ref.shape
    step, mean_util, norms = moved(2, peaks_ref, state_ref)
    usable = state_ref[1]
    weight_columns(jnp.where(usable > 0.0, jnp.exp(mean_util), 0.0), columns_ref)
    usable_rows = as_rows(usable)
    for t in range(3):
        norms_ref[t] = jnp.max(norms[t : t + 1, :])
    for d in range(rows_ref.shape[0]):
        rows = rows_ref[d, 0:8, :] + step * rows_ref[d, 8:16, :]
        mean_ref[d * own : (d + 1) * own, :] = rows[0:own, 0:slots]
    below = lax.broadcasted_iota(jnp.int32, (64 - slots, 128), 0)
    padding = jnp.where(below == 0, 1.0, 0.0)

    inverse_rows(columns_ref, raised_ref, parts_ref, inverse_ref)
    groups = draws // 128

    def chances(m, both_ref):
        inverses = inverse_ref.at[pl.ds(m * groups, groups)]
        for u in range(groups):
            g = 128 * u
            chance = raised_ref[m, :, g : g + 128] * columns_ref[m] * inverses[u : u + 1, :]
            padded = jnp.concatenate([chance, padding], axis=0)
            high = padded.astype(jnp.bfloat16)
            both_ref[0:64, g : g + 128] = high
            both_ref[64:128, g : g + 128] = (padded - high.astype(jnp.float32)).astype(jnp.bfloat16)

    def products(m, both_ref):
        for half in (0, 64):
            product_ref[m, half : half + 64, :] = lax.dot_general(
                both_ref[half : half + 64, :],
                both_ref[0:64, :],
                (((1,), (1,)), ((), ())),
                preferred_element_type=jnp.float32,
            )

    def pair(p, carry):
        products(2 * p, even_ref)
        chances(2 * p + 1, odd_ref)
        products(2 * p + 1, odd_ref)
        chances(2 * p + 2, even_ref)
        return carry

    chances(0, even_ref)
    lax.fori_loop(0, own // 2 - 1, pair, 0)
    products(own - 2, even_ref)
    chances(own - 1, odd_ref)
    products(own - 1, odd_ref)
    row = lax.broadcasted_iota(jnp.int32, (slots, slots), 0)
    col = lax.broadcasted_iota(jnp.int32, (slots, slots), 1)
    identity = jnp.where(row == col, 1.0, 0.0)
    for m in range(own):
        product = product_ref[m]
        crossed = product[64:128]
        cross = (product[0:64] + crossed + jnp.transpose(crossed))[0:slots, 0:slots]
        shares = (product[0:64] + crossed)[0:slots, slots : slots + 1]
        valid = column(usable, m, slots) > 0.0
        paired = valid & (usable_rows[m : m + 1, 0:slots] > 0.0)
        divisor = jnp.where(valid, shares, 1.0)
        jacobian_ref[m] = jnp.where(paired, identity - cross / divisor, 0.0)


def contract(x_char, nu_draws, coef_sigma, log_share, counts):
    markets, slots = log_share.shape
    depth, span = nu_draws.shape[1:]
    draw_count, mkt_count, every = (lax.axis_size(axis) for axis in ("draw", "mkt", EVERY))
    own = markets // draw_count
    draws = span * draw_count
    f32, bf16 = jnp.float32, jnp.bfloat16
    shape = lambda *sizes: jax.ShapeDtypeStruct(sizes, f32)
    state_shape = shape(5, slots, 8)
    columns = pltpu.VMEM((own, slots, 128), f32)
    units = own * draws // 128
    eight = [pltpu.VMEM((8 * units, 128), f32), pltpu.VMEM((units, 128), f32)]

    def exchange(array, distance):
        return lax.ppermute(array, "draw", [(d, d ^ distance) for d in range(draw_count)])

    def peaks_of(peak, axis):
        count = peak.shape[0]
        return lax.all_to_all(peak.reshape(count, 1, 128), axis, 0, 0, tiled=True).reshape(count, 128)

    partner = exchange(nu_draws, 1)
    x_rows, sigma, nu_hbm = in_hbm(jnp.transpose(x_char, (0, 2, 1))), in_hbm(coef_sigma), in_hbm(nu_draws)
    all_state, sums, nu_near, left = pl.pallas_call(
        start_kernel,
        out_shape=(shape(3, slots, 128), shape(draw_count, 32, 128), shape(markets, depth, span), jax.ShapeDtypeStruct((own, slots, 6 * depth), bf16)),
        in_specs=[HBM] * 5,
        out_specs=(VMEM,) * 4,
        scratch_shapes=[
            pltpu.SMEM((markets,), jnp.int32),
            pltpu.SMEM((depth,), f32),
            pltpu.VMEM((128, 128), f32),
            pltpu.VMEM((markets, slots), f32),
            pltpu.VMEM((markets, depth, slots), f32),
            pltpu.VMEM((markets, slots, 6 * depth), bf16),
            pltpu.VMEM((markets, slots, span), f32),
            pltpu.VMEM((markets, slots, 128), f32),
            pltpu.VMEM((markets, slots, 128), f32),
            *eight,
            pltpu.SemaphoreType.DMA((8,)),
        ],
        compiler_params=params(),
        name="start",
    )(in_hbm(counts), sigma, in_hbm(log_share), x_rows, nu_hbm)
    sends = pl.pallas_call(
        stage_kernel,
        out_shape=(shape(2, own, depth, span),) * 3,
        in_specs=[VMEM] * 2,
        out_specs=(VMEM,) * 3,
        compiler_params=params(),
        name="stage",
    )(nu_near, partner)
    received = []
    for k, send in enumerate(sends):
        received.append(exchange(send, 2 * (k + 1)))
    sums = lax.all_to_all(sums, "draw", 0, 0, tiled=True)
    kept = pl.pallas_call(
        lambda *refs: keep_kernel(own, *refs),
        out_shape=shape(3, slots, 8),
        in_specs=[VMEM],
        out_specs=VMEM,
        compiler_params=params(),
        name="keep",
    )(all_state)
    state, peak = pl.pallas_call(
        lambda *refs: change_kernel(1.0 / draws, own, *refs),
        out_shape=(state_shape, shape(mkt_count, 128)),
        in_specs=[VMEM] * 3,
        out_specs=(VMEM,) * 2,
        compiler_params=params(),
        name="change",
    )(sums, all_state, kept)
    peaks = peaks_of(peak, "mkt")
    raised, state, peak = pl.pallas_call(
        second_kernel,
        out_shape=(shape(own, slots, draws), state_shape, shape(every, 128)),
        in_specs=[VMEM] * 8,
        out_specs=(VMEM,) * 3,
        scratch_shapes=[columns, columns, *eight],
        compiler_params=params(),
        name="second",
    )(peaks, state, left, nu_near, partner, *received)
    state, rows = pl.pallas_call(
        third_kernel,
        out_shape=(state_shape, shape(draw_count, 16, 128)),
        in_specs=[VMEM] * 3,
        out_specs=(VMEM,) * 2,
        scratch_shapes=[columns, columns, *eight],
        compiler_params=params(),
        name="third",
    )(peaks_of(peak, EVERY), state, raised)
    rows = lax.all_to_all(rows, "draw", 0, 0, tiled=True)
    peak = pl.pallas_call(
        join_kernel,
        out_shape=shape(mkt_count, 128),
        in_specs=[VMEM],
        out_specs=VMEM,
        compiler_params=params(),
        name="join",
    )(rows)
    jacobian, mean_util, norms = pl.pallas_call(
        final_kernel,
        out_shape=(shape(own, slots, slots), shape(markets, slots), shape(3)),
        in_specs=[VMEM] * 4,
        out_specs=(VMEM, VMEM, SMEM),
        scratch_shapes=[pltpu.VMEM((128, draws), bf16)] * 2 + [columns, pltpu.VMEM((own, 128, 64), f32), *eight],
        compiler_params=params(),
        name="final",
    )(peaks_of(peak, "mkt"), state, rows, raised)
    return (mean_util, jacobian, norms)


def solution(mesh):
    return jax.shard_map(
        contract,
        mesh=mesh,
        in_specs=(P("mkt", None, None), P("mkt", None, "draw"), P(), P("mkt", None), P("mkt")),
        out_specs=(P("mkt", None), P(("mkt", "draw"), None, None), P()),
        check_vma=False,
    )
```

```python
import jax
import jax.numpy as jnp
from jax import lax
from jax.experimental import pallas as pl
from jax.experimental.pallas import tpu as pltpu
from jax.sharding import PartitionSpec as P

step_cap = 0.25
epsilon = 1e-06
LOG2E = 1.4426950408889634
VMEM = pl.BlockSpec(memory_space=pltpu.VMEM)
HBM = pl.BlockSpec(memory_space=pltpu.HBM)
SMEM = pl.BlockSpec(memory_space=pltpu.SMEM)
EVERY = ("mkt", "draw")


def pieces(value):
    high = value.astype(jnp.bfloat16).astype(jnp.float32)
    rest = value - high
    middle = rest.astype(jnp.bfloat16).astype(jnp.float32)
    return high, middle, rest - middle


def in_hbm(array):
    return pltpu.with_memory_space_constraint(array, pltpu.HBM)


def params(mebibytes=16):
    return pltpu.CompilerParams(vmem_limit_bytes=mebibytes << 20)


def column(value, slot, lanes=128):
    return jnp.broadcast_to(value[:, slot : slot + 1], (value.shape[0], lanes))


def fill(ref, value):
    largest = jnp.max(jnp.max(jnp.abs(value), axis=0, keepdims=True), axis=1, keepdims=True)
    tile = jnp.broadcast_to(largest, (8, ref.shape[1]))
    for row in range(0, ref.shape[0], 8):
        ref[row : row + 8, :] = tile


def both_starts(copies):
    for copy in copies:
        copy.start()
    return copies


def sigma_levels(sigma_ref, depth, slots):
    level = lax.broadcasted_iota(jnp.int32, (depth, slots), 0)
    sigma = jnp.zeros((depth, slots), jnp.float32)
    for k in range(depth):
        sigma = jnp.where(level == k, sigma_ref[k], sigma)
    return sigma * LOG2E


def left_side(scaled):
    high, middle, low = pieces(scaled)
    left = jnp.concatenate([high, high, middle, high, low, middle], axis=0)
    return jnp.transpose(left.astype(jnp.bfloat16))


def raise_tastes(left, draws):
    high, middle, low = pieces(draws)
    right = jnp.concatenate([high, middle, high, low, high, middle], axis=0)
    return jnp.exp2(jnp.dot(left, right.astype(jnp.bfloat16), preferred_element_type=jnp.float32))


def usable_weights(state_ref, mean_util):
    return jnp.where(state_ref[1] > 0.0, jnp.exp(mean_util), 0.0)


def send_copies(sums_ref, sums):
    for d in range(sums_ref.shape[0]):
        sums_ref[d] = sums


def weight_columns(weights, columns_ref):
    for m in range(columns_ref.shape[0]):
        columns_ref[m] = column(weights, m)


def inverse_rows(columns_ref, raised_ref, parts_ref, inverse_ref):
    markets, slots, draws = raised_ref.shape
    units = [(m, g) for m in range(markets) for g in range(0, draws, 128)]
    for u, (m, g) in enumerate(units):
        part = raised_ref[m, 0:8, g : g + 128] * columns_ref[m, 0:8, :]
        for j in range(8, slots, 8):
            part = part + raised_ref[m, j : j + 8, g : g + 128] * columns_ref[m, j : j + 8, :]
        parts_ref[8 * u : 8 * u + 8, :] = part
    for u in range(0, len(units), 8):
        below = parts_ref[pl.ds(8 * u, 8, stride=8), :] + 1.0
        for j in range(1, 8):
            below = below + parts_ref[pl.ds(8 * u + j, 8, stride=8), :]
        inverse_ref[u : u + 8, :] = 1.0 / below


def totals_over(columns_ref, raised_ref, parts_ref, inverse_ref, totals_ref):
    markets, slots, draws = raised_ref.shape
    inverse_rows(columns_ref, raised_ref, parts_ref, inverse_ref)
    groups = draws // 128
    for m in range(markets):
        total = jnp.zeros((slots, 128), jnp.float32)
        for g in range(groups):
            u = m * groups + g
            total = total + raised_ref[m, :, 128 * g : 128 * g + 128] * inverse_ref[u : u + 1, :]
        totals_ref[m] = total


def send_lane_sums(sums_ref, totals_ref):
    markets, slots = totals_ref.shape[:2]
    lane = lax.broadcasted_iota(jnp.int32, (slots, 128), 1)
    ones = jnp.ones((256, 128), jnp.bfloat16)
    sums = jnp.zeros((slots, 128), jnp.float32)
    for m in range(markets):
        total = totals_ref[m]
        high = total.astype(jnp.bfloat16)
        low = (total - high.astype(jnp.float32)).astype(jnp.bfloat16)
        both = jnp.concatenate([high, low], axis=1)
        sums = jnp.where(lane == m, jnp.dot(both, ones, preferred_element_type=jnp.float32), sums)
    rest = jnp.concatenate([sums[32:slots], jnp.zeros((64 - slots, 128), jnp.float32)], axis=0)
    send_copies(sums_ref, jnp.where(lane[0:32] < 64, sums[0:32], pltpu.roll(rest, 64, axis=1)))


def start_kernel(counts_hbm, sigma_hbm, log_share_hbm, x_hbm, nu_hbm, state_ref, sums_ref, nu_ref, kept_ref, counts_ref, sigma_ref, rows_ref, log_share_ref, x_ref, left_ref, raised_ref, columns_ref, totals_ref, parts_ref, inverse_ref, sems):
    markets, slots = log_share_hbm.shape
    depth = x_hbm.shape[1]
    chunk = markets // 4
    small = both_starts(
        [
            pltpu.make_async_copy(x_hbm, x_ref, sems.at[0]),
            pltpu.make_async_copy(sigma_hbm, sigma_ref, sems.at[1]),
            pltpu.make_async_copy(log_share_hbm, log_share_ref, sems.at[2]),
            pltpu.make_async_copy(counts_hbm, counts_ref, sems.at[3]),
        ]
    )
    large = both_starts(
        [
            pltpu.make_async_copy(nu_hbm.at[pl.ds(c * chunk, chunk)], nu_ref.at[pl.ds(c * chunk, chunk)], sems.at[4 + c])
            for c in range(4)
        ]
    )
    rows_ref[...] = jnp.zeros_like(rows_ref)
    for copy in small:
        copy.wait()
    sigma = sigma_levels(sigma_ref, depth, slots)
    for m in range(markets):
        left_ref[m] = left_side(x_ref[m] * sigma)
    base = lax.axis_index("draw") * kept_ref.shape[0]
    for m in range(kept_ref.shape[0]):
        kept_ref[m] = left_ref[base + m]
    rows_ref[0:markets, 0:slots] = log_share_ref[...]
    log_share = jnp.transpose(rows_ref[...])[0:slots, :]
    slot = lax.broadcasted_iota(jnp.int32, (slots, 128), 0)
    lane = lax.broadcasted_iota(jnp.int32, (8, 128), 1)
    count = jnp.zeros((8, 128), jnp.int32)
    for m in range(markets):
        count = jnp.where(lane == m, counts_ref[m], count)
    usable = slot < jnp.broadcast_to(count[0:1, :], (slots, 128))
    inside = jnp.sum(jnp.where(usable, jnp.exp(log_share), 0.0), axis=0, keepdims=True)
    mean_util = jnp.where(usable, log_share - jnp.log(1.0 - inside), 0.0)
    state_ref[0] = log_share
    state_ref[1] = jnp.where(usable, 1.0, 0.0)
    state_ref[2] = mean_util
    weight_columns(jnp.where(usable, jnp.exp(mean_util), 0.0), columns_ref)
    for copy in large:
        copy.wait()
    for m in range(markets):
        raised_ref[m] = raise_tastes(left_ref[m], nu_ref[m])
    totals_over(columns_ref, raised_ref, parts_ref, inverse_ref, totals_ref)
    send_lane_sums(sums_ref, totals_ref)


def stage_kernel(nu_ref, partner_ref, *sends):
    own = sends[0].shape[1]
    mine = lax.axis_index("draw")
    for k, send in enumerate(sends):
        first = (mine ^ (2 * (k + 1))) * own
        for m in range(own):
            send[0, m] = nu_ref[first + m]
            send[1, m] = partner_ref[first + m]


def keep_kernel(own, all_ref, kept_ref):
    slots = all_ref.shape[1]
    shift = 128 - lax.axis_index("draw") * own
    kept = lax.broadcasted_iota(jnp.int32, (slots, 8), 1) < own
    for p in range(3):
        kept_ref[p] = jnp.where(kept, pltpu.roll(all_ref[p], shift, axis=1)[:, 0:8], 0.0)


def change_kernel(inverse, own, sums_ref, all_ref, kept_ref, state_ref, peak_ref):
    mine = lax.axis_index("draw")
    total = sums_ref[0]
    for d in range(1, sums_ref.shape[0]):
        total = total + sums_ref[d]
    slots = all_ref.shape[1]
    sums = jnp.concatenate([total, pltpu.roll(total, 64, axis=1)[0 : slots - 32]], axis=0)
    usable = all_ref[1] > 0.0
    shares = sums * usable_weights(all_ref, all_ref[2]) * inverse
    change = jnp.where(usable, all_ref[0] - jnp.log(jnp.where(usable, shares, 1.0)), 0.0)
    fill(peak_ref, change)
    kept = lax.broadcasted_iota(jnp.int32, (slots, 8), 1) < own
    for p in range(3):
        state_ref[p] = kept_ref[p]
    state_ref[3] = jnp.where(kept, pltpu.roll(change, 128 - mine * own, axis=1)[:, 0:8], 0.0)
    state_ref[4] = jnp.zeros((slots, 8), jnp.float32)


def moved(turn, peaks_ref, state_ref):
    largest = jnp.max(peaks_ref[...], axis=0, keepdims=True)
    step = jnp.minimum(1.0, step_cap / (largest + epsilon))
    row = lax.broadcasted_iota(jnp.int32, state_ref.shape[1:], 0)
    width = state_ref.shape[2]
    norms = jnp.where(row == turn, largest[:, 0:width], state_ref[4])
    return step, state_ref[2] + step[:, 0:width] * state_ref[3], norms


def next_change(turn, peaks_ref, state_ref, out_ref, raised_ref, columns_ref, totals_ref, *eight):
    own, _, draws = raised_ref.shape
    _, mean_util, norms = moved(turn, peaks_ref, state_ref)
    usable = state_ref[1] > 0.0
    weights = jnp.where(usable, jnp.exp(mean_util), 0.0)
    weight_columns(weights, columns_ref)
    totals_over(columns_ref, raised_ref, *eight, totals_ref)
    lane = lax.broadcasted_iota(jnp.int32, weights.shape, 1)
    sums = jnp.ones(weights.shape, jnp.float32)
    for m in range(own):
        sums = jnp.where(lane == m, jnp.sum(totals_ref[m], axis=1, keepdims=True), sums)
    shares = sums * weights * (1.0 / draws)
    change = jnp.where(usable, state_ref[0] - jnp.log(jnp.where(usable, shares, 1.0)), 0.0)
    out_ref[0] = state_ref[0]
    out_ref[1] = state_ref[1]
    out_ref[2] = mean_util
    out_ref[3] = change
    out_ref[4] = norms
    return mean_util, change


def second_kernel(peaks_ref, state_ref, left_ref, nu_ref, partner_ref, *refs):
    received = refs[:3]
    raised_ref, out_ref, peak_ref, *scratch = refs[3:]
    own = raised_ref.shape[0]
    base = lax.axis_index("draw") * own
    sources = [nu_ref.at[pl.ds(base, own)], partner_ref.at[pl.ds(base, own)]]
    for ref in received:
        sources += [ref.at[0], ref.at[1]]
    span = nu_ref.shape[2]
    for m in range(own):
        for s, source in enumerate(sources):
            raised_ref[m, :, s * span : (s + 1) * span] = raise_tastes(left_ref[m], source[m])
    _, change = next_change(0, peaks_ref, state_ref, out_ref, raised_ref, *scratch)
    fill(peak_ref, change)


def as_rows(value):
    padded = jnp.concatenate([value, jnp.zeros((128 - value.shape[0], 8), jnp.float32)], axis=0)
    return jnp.transpose(padded)


def third_kernel(peaks_ref, state_ref, raised_ref, out_ref, rows_ref, *scratch):
    mean_util, change = next_change(1, peaks_ref, state_ref, out_ref, raised_ref, *scratch)
    send_copies(rows_ref, jnp.concatenate([as_rows(mean_util), as_rows(change)], axis=0))


def join_kernel(rows_ref, peak_ref):
    largest = jnp.abs(rows_ref[0, 8:16, :])
    for d in range(1, rows_ref.shape[0]):
        largest = jnp.maximum(largest, jnp.abs(rows_ref[d, 8:16, :]))
    fill(peak_ref, largest)


def final_kernel(peaks_ref, state_ref, rows_ref, raised_ref, jacobian_hbm, mean_hbm, norms_ref, jacobian_ref, mean_ref, sems, even_ref, odd_ref, columns_ref, product_ref, parts_ref, inverse_ref):
    own, slots, draws = raised_ref.shape
    step, mean_util, norms = moved(2, peaks_ref, state_ref)
    usable = state_ref[1]
    weight_columns(jnp.where(usable > 0.0, jnp.exp(mean_util), 0.0), columns_ref)
    usable_rows = as_rows(usable)
    for t in range(3):
        norms_ref[t] = jnp.max(norms[t : t + 1, :])
    for d in range(rows_ref.shape[0]):
        rows = rows_ref[d, 0:8, :] + step * rows_ref[d, 8:16, :]
        mean_ref[d * own : (d + 1) * own, :] = rows[0:own, 0:slots]
    copies = both_starts([pltpu.make_async_copy(mean_ref, mean_hbm, sems.at[own])])
    below = lax.broadcasted_iota(jnp.int32, (64 - slots, 128), 0)
    padding = jnp.where(below == 0, 1.0, 0.0)

    inverse_rows(columns_ref, raised_ref, parts_ref, inverse_ref)
    groups = draws // 128

    def chances(m, both_ref):
        inverses = inverse_ref.at[pl.ds(m * groups, groups)]
        for u in range(groups):
            g = 128 * u
            chance = raised_ref[m, :, g : g + 128] * columns_ref[m] * inverses[u : u + 1, :]
            padded = jnp.concatenate([chance, padding], axis=0)
            high = padded.astype(jnp.bfloat16)
            both_ref[0:64, g : g + 128] = high
            both_ref[64:128, g : g + 128] = (padded - high.astype(jnp.float32)).astype(jnp.bfloat16)

    def products(m, both_ref):
        for half in (0, 64):
            product_ref[m, half : half + 64, :] = lax.dot_general(
                both_ref[half : half + 64, :],
                both_ref[0:64, :],
                (((1,), (1,)), ((), ())),
                preferred_element_type=jnp.float32,
            )

    def pair(p, carry):
        products(2 * p, even_ref)
        chances(2 * p + 1, odd_ref)
        products(2 * p + 1, odd_ref)
        chances(2 * p + 2, even_ref)
        return carry

    chances(0, even_ref)
    lax.fori_loop(0, own // 2 - 1, pair, 0)
    products(own - 2, even_ref)
    chances(own - 1, odd_ref)
    products(own - 1, odd_ref)
    row = lax.broadcasted_iota(jnp.int32, (slots, slots), 0)
    col = lax.broadcasted_iota(jnp.int32, (slots, slots), 1)
    identity = jnp.where(row == col, 1.0, 0.0)
    for m in range(own):
        product = product_ref[m]
        crossed = product[64:128]
        cross = (product[0:64] + crossed + jnp.transpose(crossed))[0:slots, 0:slots]
        shares = (product[0:64] + crossed)[0:slots, slots : slots + 1]
        valid = column(usable, m, slots) > 0.0
        paired = valid & (usable_rows[m : m + 1, 0:slots] > 0.0)
        divisor = jnp.where(valid, shares, 1.0)
        jacobian_ref[m] = jnp.where(paired, identity - cross / divisor, 0.0)
        copies += both_starts([pltpu.make_async_copy(jacobian_ref.at[m], jacobian_hbm.at[m], sems.at[m])])
    for copy in copies:
        copy.wait()


def contract(x_char, nu_draws, coef_sigma, log_share, counts):
    markets, slots = log_share.shape
    depth, span = nu_draws.shape[1:]
    draw_count, mkt_count, every = (lax.axis_size(axis) for axis in ("draw", "mkt", EVERY))
    own = markets // draw_count
    draws = span * draw_count
    f32, bf16 = jnp.float32, jnp.bfloat16
    shape = lambda *sizes: jax.ShapeDtypeStruct(sizes, f32)
    state_shape = shape(5, slots, 8)
    columns = pltpu.VMEM((own, slots, 128), f32)
    units = own * draws // 128
    eight = [pltpu.VMEM((8 * units, 128), f32), pltpu.VMEM((units, 128), f32)]

    def exchange(array, distance):
        return lax.ppermute(array, "draw", [(d, d ^ distance) for d in range(draw_count)])

    def peaks_of(peak, axis):
        count = peak.shape[0]
        return lax.all_to_all(peak.reshape(count, 1, 128), axis, 0, 0, tiled=True).reshape(count, 128)

    partner = exchange(nu_draws, 1)
    x_rows, sigma, nu_hbm = in_hbm(jnp.transpose(x_char, (0, 2, 1))), in_hbm(coef_sigma), in_hbm(nu_draws)
    all_state, sums, nu_near, left = pl.pallas_call(
        start_kernel,
        out_shape=(shape(3, slots, 128), shape(draw_count, 32, 128), shape(markets, depth, span), jax.ShapeDtypeStruct((own, slots, 6 * depth), bf16)),
        in_specs=[HBM] * 5,
        out_specs=(VMEM,) * 4,
        scratch_shapes=[
            pltpu.SMEM((markets,), jnp.int32),
            pltpu.SMEM((depth,), f32),
            pltpu.VMEM((128, 128), f32),
            pltpu.VMEM((markets, slots), f32),
            pltpu.VMEM((markets, depth, slots), f32),
            pltpu.VMEM((markets, slots, 6 * depth), bf16),
            pltpu.VMEM((markets, slots, span), f32),
            pltpu.VMEM((markets, slots, 128), f32),
            pltpu.VMEM((markets, slots, 128), f32),
            *eight,
            pltpu.SemaphoreType.DMA((8,)),
        ],
        compiler_params=params(),
        name="start",
    )(in_hbm(counts), sigma, in_hbm(log_share), x_rows, nu_hbm)
    sends = pl.pallas_call(
        stage_kernel,
        out_shape=(shape(2, own, depth, span),) * 3,
        in_specs=[VMEM] * 2,
        out_specs=(VMEM,) * 3,
        compiler_params=params(),
        name="stage",
    )(nu_near, partner)
    received = []
    for k, send in enumerate(sends):
        received.append(exchange(send, 2 * (k + 1)))
    sums = lax.all_to_all(sums, "draw", 0, 0, tiled=True)
    kept = pl.pallas_call(
        lambda *refs: keep_kernel(own, *refs),
        out_shape=shape(3, slots, 8),
        in_specs=[VMEM],
        out_specs=VMEM,
        compiler_params=params(),
        name="keep",
    )(all_state)
    state, peak = pl.pallas_call(
        lambda *refs: change_kernel(1.0 / draws, own, *refs),
        out_shape=(state_shape, shape(mkt_count, 128)),
        in_specs=[VMEM] * 3,
        out_specs=(VMEM,) * 2,
        compiler_params=params(),
        name="change",
    )(sums, all_state, kept)
    peaks = peaks_of(peak, "mkt")
    raised, state, peak = pl.pallas_call(
        second_kernel,
        out_shape=(shape(own, slots, draws), state_shape, shape(every, 128)),
        in_specs=[VMEM] * 8,
        out_specs=(VMEM,) * 3,
        scratch_shapes=[columns, columns, *eight],
        compiler_params=params(),
        name="second",
    )(peaks, state, left, nu_near, partner, *received)
    state, rows = pl.pallas_call(
        third_kernel,
        out_shape=(state_shape, shape(draw_count, 16, 128)),
        in_specs=[VMEM] * 3,
        out_specs=(VMEM,) * 2,
        scratch_shapes=[columns, columns, *eight],
        compiler_params=params(),
        name="third",
    )(peaks_of(peak, EVERY), state, raised)
    rows = lax.all_to_all(rows, "draw", 0, 0, tiled=True)
    peak = pl.pallas_call(
        join_kernel,
        out_shape=shape(mkt_count, 128),
        in_specs=[VMEM],
        out_specs=VMEM,
        compiler_params=params(),
        name="join",
    )(rows)
    jacobian, mean_util, norms = pl.pallas_call(
        final_kernel,
        out_shape=(shape(own, slots, slots), shape(markets, slots), shape(3)),
        in_specs=[VMEM] * 4,
        out_specs=(HBM, HBM, SMEM),
        scratch_shapes=[
            pltpu.VMEM((own, slots, slots), f32),
            pltpu.VMEM((markets, slots), f32),
            pltpu.SemaphoreType.DMA((own + 1,)),
        ]
        + [pltpu.VMEM((128, draws), bf16)] * 2 + [columns, pltpu.VMEM((own, 128, 64), f32), *eight],
        compiler_params=params(),
        name="final",
    )(peaks_of(peak, "mkt"), state, rows, raised)
    return (mean_util, jacobian, norms)


def solution(mesh):
    return jax.shard_map(
        contract,
        mesh=mesh,
        in_specs=(P("mkt", None, None), P("mkt", None, "draw"), P(), P("mkt", None), P("mkt")),
        out_specs=(P("mkt", None), P(("mkt", "draw"), None, None), P()),
        check_vma=False,
    )
```

```python
import jax
import jax.numpy as jnp
from jax import lax
from jax.experimental import pallas as pl
from jax.experimental.pallas import tpu as pltpu
from jax.sharding import PartitionSpec as P

step_cap = 0.25
epsilon = 1e-06
LOG2E = 1.4426950408889634
VMEM = pl.BlockSpec(memory_space=pltpu.VMEM)
HBM = pl.BlockSpec(memory_space=pltpu.HBM)
SMEM = pl.BlockSpec(memory_space=pltpu.SMEM)
EVERY = ("mkt", "draw")


def pieces(value):
    high = value.astype(jnp.bfloat16).astype(jnp.float32)
    rest = value - high
    middle = rest.astype(jnp.bfloat16).astype(jnp.float32)
    return high, middle, rest - middle


def in_hbm(array):
    return pltpu.with_memory_space_constraint(array, pltpu.HBM)


def params(mebibytes=16):
    return pltpu.CompilerParams(vmem_limit_bytes=mebibytes << 20)


def column(value, slot, lanes=128):
    return jnp.broadcast_to(value[:, slot : slot + 1], (value.shape[0], lanes))


def fill(ref, value):
    largest = jnp.max(jnp.max(jnp.abs(value), axis=0, keepdims=True), axis=1, keepdims=True)
    tile = jnp.broadcast_to(largest, (8, ref.shape[1]))
    for row in range(0, ref.shape[0], 8):
        ref[row : row + 8, :] = tile


def both_starts(copies):
    for copy in copies:
        copy.start()
    return copies


def sigma_levels(sigma_ref, depth, slots):
    level = lax.broadcasted_iota(jnp.int32, (depth, slots), 0)
    sigma = jnp.zeros((depth, slots), jnp.float32)
    for k in range(depth):
        sigma = jnp.where(level == k, sigma_ref[k], sigma)
    return sigma * LOG2E


def left_side(scaled):
    high, middle, low = pieces(scaled)
    left = jnp.concatenate([high, high, middle, high, low, middle], axis=0)
    return jnp.transpose(left.astype(jnp.bfloat16))


def raise_tastes(left, draws):
    high, middle, low = pieces(draws)
    right = jnp.concatenate([high, middle, high, low, high, middle], axis=0)
    return jnp.exp2(jnp.dot(left, right.astype(jnp.bfloat16), preferred_element_type=jnp.float32))


def usable_weights(state_ref, mean_util):
    return jnp.where(state_ref[1] > 0.0, jnp.exp(mean_util), 0.0)


def send_copies(sums_ref, sums):
    for d in range(sums_ref.shape[0]):
        sums_ref[d] = sums


def weight_columns(weights, columns_ref):
    for m in range(columns_ref.shape[0]):
        columns_ref[m] = column(weights, m)


def inverse_rows(columns_ref, raised_ref, parts_ref, inverse_ref):
    markets, slots, draws = raised_ref.shape
    units = [(m, g) for m in range(markets) for g in range(0, draws, 128)]
    for u, (m, g) in enumerate(units):
        part = raised_ref[m, 0:8, g : g + 128] * columns_ref[m, 0:8, :]
        for j in range(8, slots, 8):
            part = part + raised_ref[m, j : j + 8, g : g + 128] * columns_ref[m, j : j + 8, :]
        parts_ref[8 * u : 8 * u + 8, :] = part
    for u in range(0, len(units), 8):
        below = parts_ref[pl.ds(8 * u, 8, stride=8), :] + 1.0
        for j in range(1, 8):
            below = below + parts_ref[pl.ds(8 * u + j, 8, stride=8), :]
        inverse_ref[u : u + 8, :] = 1.0 / below


def totals_over(columns_ref, raised_ref, parts_ref, inverse_ref, totals_ref):
    markets, slots, draws = raised_ref.shape
    inverse_rows(columns_ref, raised_ref, parts_ref, inverse_ref)
    groups = draws // 128
    for m in range(markets):
        total = jnp.zeros((slots, 128), jnp.float32)
        for g in range(groups):
            u = m * groups + g
            total = total + raised_ref[m, :, 128 * g : 128 * g + 128] * inverse_ref[u : u + 1, :]
        totals_ref[m] = total


def send_lane_sums(sums_ref, totals_ref):
    markets, slots = totals_ref.shape[:2]
    lane = lax.broadcasted_iota(jnp.int32, (slots, 128), 1)
    ones = jnp.ones((256, 128), jnp.bfloat16)
    sums = jnp.zeros((slots, 128), jnp.float32)
    for m in range(markets):
        total = totals_ref[m]
        high = total.astype(jnp.bfloat16)
        low = (total - high.astype(jnp.float32)).astype(jnp.bfloat16)
        both = jnp.concatenate([high, low], axis=1)
        sums = jnp.where(lane == m, jnp.dot(both, ones, preferred_element_type=jnp.float32), sums)
    rest = jnp.concatenate([sums[32:slots], jnp.zeros((64 - slots, 128), jnp.float32)], axis=0)
    send_copies(sums_ref, jnp.where(lane[0:32] < 64, sums[0:32], pltpu.roll(rest, 64, axis=1)))


def start_kernel(counts_hbm, sigma_hbm, log_share_hbm, x_hbm, nu_hbm, state_ref, sums_ref, nu_ref, kept_ref, counts_ref, sigma_ref, rows_ref, log_share_ref, x_ref, left_ref, raised_ref, columns_ref, totals_ref, parts_ref, inverse_ref, sems):
    markets, slots = log_share_hbm.shape
    depth = x_hbm.shape[1]
    chunk = markets // 4
    small = both_starts(
        [
            pltpu.make_async_copy(x_hbm, x_ref, sems.at[0]),
            pltpu.make_async_copy(sigma_hbm, sigma_ref, sems.at[1]),
            pltpu.make_async_copy(log_share_hbm, log_share_ref, sems.at[2]),
            pltpu.make_async_copy(counts_hbm, counts_ref, sems.at[3]),
        ]
    )
    large = both_starts(
        [
            pltpu.make_async_copy(nu_hbm.at[pl.ds(c * chunk, chunk)], nu_ref.at[pl.ds(c * chunk, chunk)], sems.at[4 + c])
            for c in range(4)
        ]
    )
    rows_ref[...] = jnp.zeros_like(rows_ref)
    for copy in small:
        copy.wait()
    sigma = sigma_levels(sigma_ref, depth, slots)
    for m in range(markets):
        left_ref[m] = left_side(x_ref[m] * sigma)
    base = lax.axis_index("draw") * kept_ref.shape[0]
    for m in range(kept_ref.shape[0]):
        kept_ref[m] = left_ref[base + m]
    rows_ref[0:markets, 0:slots] = log_share_ref[...]
    log_share = jnp.transpose(rows_ref[...])[0:slots, :]
    slot = lax.broadcasted_iota(jnp.int32, (slots, 128), 0)
    lane = lax.broadcasted_iota(jnp.int32, (8, 128), 1)
    count = jnp.zeros((8, 128), jnp.int32)
    for m in range(markets):
        count = jnp.where(lane == m, counts_ref[m], count)
    usable = slot < jnp.broadcast_to(count[0:1, :], (slots, 128))
    inside = jnp.sum(jnp.where(usable, jnp.exp(log_share), 0.0), axis=0, keepdims=True)
    mean_util = jnp.where(usable, log_share - jnp.log(1.0 - inside), 0.0)
    state_ref[0] = log_share
    state_ref[1] = jnp.where(usable, 1.0, 0.0)
    state_ref[2] = mean_util
    weight_columns(jnp.where(usable, jnp.exp(mean_util), 0.0), columns_ref)
    for copy in large:
        copy.wait()
    for m in range(markets):
        raised_ref[m] = raise_tastes(left_ref[m], nu_ref[m])
    totals_over(columns_ref, raised_ref, parts_ref, inverse_ref, totals_ref)
    send_lane_sums(sums_ref, totals_ref)


def stage_kernel(nu_ref, partner_ref, *sends):
    own = sends[0].shape[1]
    mine = lax.axis_index("draw")
    for k, send in enumerate(sends):
        first = (mine ^ (2 * (k + 1))) * own
        for m in range(own):
            send[0, m] = nu_ref[first + m]
            send[1, m] = partner_ref[first + m]


def keep_kernel(own, all_ref, kept_ref):
    slots = all_ref.shape[1]
    shift = 128 - lax.axis_index("draw") * own
    kept = lax.broadcasted_iota(jnp.int32, (slots, 8), 1) < own
    for p in range(3):
        kept_ref[p] = jnp.where(kept, pltpu.roll(all_ref[p], shift, axis=1)[:, 0:8], 0.0)


def change_kernel(inverse, own, sums_ref, all_ref, kept_ref, state_ref, peak_ref):
    mine = lax.axis_index("draw")
    total = sums_ref[0]
    for d in range(1, sums_ref.shape[0]):
        total = total + sums_ref[d]
    slots = all_ref.shape[1]
    sums = jnp.concatenate([total, pltpu.roll(total, 64, axis=1)[0 : slots - 32]], axis=0)
    usable = all_ref[1] > 0.0
    shares = sums * usable_weights(all_ref, all_ref[2]) * inverse
    change = jnp.where(usable, all_ref[0] - jnp.log(jnp.where(usable, shares, 1.0)), 0.0)
    fill(peak_ref, change)
    kept = lax.broadcasted_iota(jnp.int32, (slots, 8), 1) < own
    for p in range(3):
        state_ref[p] = kept_ref[p]
    state_ref[3] = jnp.where(kept, pltpu.roll(change, 128 - mine * own, axis=1)[:, 0:8], 0.0)
    state_ref[4] = jnp.zeros((slots, 8), jnp.float32)


def moved(turn, peaks_ref, state_ref):
    largest = jnp.max(peaks_ref[...], axis=0, keepdims=True)
    step = jnp.minimum(1.0, step_cap / (largest + epsilon))
    row = lax.broadcasted_iota(jnp.int32, state_ref.shape[1:], 0)
    width = state_ref.shape[2]
    norms = jnp.where(row == turn, largest[:, 0:width], state_ref[4])
    return step, state_ref[2] + step[:, 0:width] * state_ref[3], norms


def next_change(turn, peaks_ref, state_ref, out_ref, raised_ref, columns_ref, totals_ref, *eight):
    own, _, draws = raised_ref.shape
    _, mean_util, norms = moved(turn, peaks_ref, state_ref)
    usable = state_ref[1] > 0.0
    weights = jnp.where(usable, jnp.exp(mean_util), 0.0)
    weight_columns(weights, columns_ref)
    totals_over(columns_ref, raised_ref, *eight, totals_ref)
    lane = lax.broadcasted_iota(jnp.int32, weights.shape, 1)
    sums = jnp.ones(weights.shape, jnp.float32)
    for m in range(own):
        sums = jnp.where(lane == m, jnp.sum(totals_ref[m], axis=1, keepdims=True), sums)
    shares = sums * weights * (1.0 / draws)
    change = jnp.where(usable, state_ref[0] - jnp.log(jnp.where(usable, shares, 1.0)), 0.0)
    out_ref[0] = state_ref[0]
    out_ref[1] = state_ref[1]
    out_ref[2] = mean_util
    out_ref[3] = change
    out_ref[4] = norms
    return mean_util, change


def second_kernel(peaks_ref, state_ref, left_ref, nu_ref, partner_ref, *refs):
    received = refs[:3]
    raised_ref, out_ref, peak_ref, *scratch = refs[3:]
    own = raised_ref.shape[0]
    base = lax.axis_index("draw") * own
    sources = [nu_ref.at[pl.ds(base, own)], partner_ref.at[pl.ds(base, own)]]
    for ref in received:
        sources += [ref.at[0], ref.at[1]]
    span = nu_ref.shape[2]
    for m in range(own):
        for s, source in enumerate(sources):
            raised_ref[m, :, s * span : (s + 1) * span] = raise_tastes(left_ref[m], source[m])
    _, change = next_change(0, peaks_ref, state_ref, out_ref, raised_ref, *scratch)
    fill(peak_ref, change)


def as_rows(value):
    padded = jnp.concatenate([value, jnp.zeros((128 - value.shape[0], 8), jnp.float32)], axis=0)
    return jnp.transpose(padded)


def third_kernel(peaks_ref, state_ref, raised_ref, out_ref, rows_ref, *scratch):
    mean_util, change = next_change(1, peaks_ref, state_ref, out_ref, raised_ref, *scratch)
    send_copies(rows_ref, jnp.concatenate([as_rows(mean_util), as_rows(change)], axis=0))


def join_kernel(rows_ref, peak_ref):
    largest = jnp.abs(rows_ref[0, 8:16, :])
    for d in range(1, rows_ref.shape[0]):
        largest = jnp.maximum(largest, jnp.abs(rows_ref[d, 8:16, :]))
    fill(peak_ref, largest)


def final_kernel(peaks_ref, state_ref, rows_ref, raised_ref, jacobian_ref, mean_ref, norms_ref, even_ref, odd_ref, columns_ref, product_ref, parts_ref, inverse_ref):
    own, slots, draws = raised_ref.shape
    step, mean_util, norms = moved(2, peaks_ref, state_ref)
    usable = state_ref[1]
    weight_columns(jnp.where(usable > 0.0, jnp.exp(mean_util), 0.0), columns_ref)
    usable_rows = as_rows(usable)
    for t in range(3):
        norms_ref[t] = jnp.max(norms[t : t + 1, :])
    for d in range(rows_ref.shape[0]):
        rows = rows_ref[d, 0:8, :] + step * rows_ref[d, 8:16, :]
        mean_ref[d * own : (d + 1) * own, :] = rows[0:own, 0:slots]
    below = lax.broadcasted_iota(jnp.int32, (64 - slots, 128), 0)
    padding = jnp.where(below == 0, 1.0, 0.0)

    inverse_rows(columns_ref, raised_ref, parts_ref, inverse_ref)
    groups = draws // 128

    def chances(m, both_ref):
        inverses = inverse_ref.at[pl.ds(m * groups, groups)]
        for u in range(groups):
            g = 128 * u
            chance = raised_ref[m, :, g : g + 128] * columns_ref[m] * inverses[u : u + 1, :]
            padded = jnp.concatenate([chance, padding], axis=0)
            high = padded.astype(jnp.bfloat16)
            both_ref[0:64, g : g + 128] = high
            both_ref[64:128, g : g + 128] = (padded - high.astype(jnp.float32)).astype(jnp.bfloat16)

    def products(m, both_ref):
        for half in (0, 64):
            product_ref[m, half : half + 64, :] = lax.dot_general(
                both_ref[half : half + 64, :],
                both_ref[0:64, :],
                (((1,), (1,)), ((), ())),
                preferred_element_type=jnp.float32,
            )

    def pair(p, carry):
        products(2 * p, even_ref)
        chances(2 * p + 1, odd_ref)
        products(2 * p + 1, odd_ref)
        chances(2 * p + 2, even_ref)
        return carry

    chances(0, even_ref)
    lax.fori_loop(0, own // 2 - 1, pair, 0)
    products(own - 2, even_ref)
    chances(own - 1, odd_ref)
    products(own - 1, odd_ref)
    row = lax.broadcasted_iota(jnp.int32, (slots, slots), 0)
    col = lax.broadcasted_iota(jnp.int32, (slots, slots), 1)
    identity = jnp.where(row == col, 1.0, 0.0)
    for m in range(own):
        product = product_ref[m]
        crossed = product[64:128]
        cross = (product[0:64] + crossed + jnp.transpose(crossed))[0:slots, 0:slots]
        shares = (product[0:64] + crossed)[0:slots, slots : slots + 1]
        valid = column(usable, m, slots) > 0.0
        paired = valid & (usable_rows[m : m + 1, 0:slots] > 0.0)
        divisor = jnp.where(valid, shares, 1.0)
        jacobian_ref[m] = jnp.where(paired, identity - cross / divisor, 0.0)


def contract(x_char, nu_draws, coef_sigma, log_share, counts):
    markets, slots = log_share.shape
    depth, span = nu_draws.shape[1:]
    draw_count, mkt_count, every = (lax.axis_size(axis) for axis in ("draw", "mkt", EVERY))
    own = markets // draw_count
    draws = span * draw_count
    f32, bf16 = jnp.float32, jnp.bfloat16
    shape = lambda *sizes: jax.ShapeDtypeStruct(sizes, f32)
    state_shape = shape(5, slots, 8)
    columns = pltpu.VMEM((own, slots, 128), f32)
    units = own * draws // 128
    eight = [pltpu.VMEM((8 * units + 64, 128), f32), pltpu.VMEM((units, 128), f32)]

    def exchange(array, distance):
        return lax.ppermute(array, "draw", [(d, d ^ distance) for d in range(draw_count)])

    def peaks_of(peak, axis):
        count = peak.shape[0]
        return lax.all_to_all(peak.reshape(count, 1, 128), axis, 0, 0, tiled=True).reshape(count, 128)

    partner = exchange(nu_draws, 1)
    x_rows, sigma, nu_hbm = in_hbm(jnp.transpose(x_char, (0, 2, 1))), in_hbm(coef_sigma), in_hbm(nu_draws)
    all_state, sums, nu_near, left = pl.pallas_call(
        start_kernel,
        out_shape=(shape(3, slots, 128), shape(draw_count, 32, 128), shape(markets, depth, span), jax.ShapeDtypeStruct((own, slots, 6 * depth), bf16)),
        in_specs=[HBM] * 5,
        out_specs=(VMEM,) * 4,
        scratch_shapes=[
            pltpu.SMEM((markets,), jnp.int32),
            pltpu.SMEM((depth,), f32),
            pltpu.VMEM((128, 128), f32),
            pltpu.VMEM((markets, slots), f32),
            pltpu.VMEM((markets, depth, slots), f32),
            pltpu.VMEM((markets, slots, 6 * depth), bf16),
            pltpu.VMEM((markets, slots, span), f32),
            pltpu.VMEM((markets, slots, 128), f32),
            pltpu.VMEM((markets, slots, 128), f32),
            *eight,
            pltpu.SemaphoreType.DMA((8,)),
        ],
        compiler_params=params(),
        name="start",
    )(in_hbm(counts), sigma, in_hbm(log_share), x_rows, nu_hbm)
    sends = pl.pallas_call(
        stage_kernel,
        out_shape=(shape(2, own, depth, span),) * 3,
        in_specs=[VMEM] * 2,
        out_specs=(VMEM,) * 3,
        compiler_params=params(),
        name="stage",
    )(nu_near, partner)
    received = []
    for k, send in enumerate(sends):
        received.append(exchange(send, 2 * (k + 1)))
    sums = lax.all_to_all(sums, "draw", 0, 0, tiled=True)
    kept = pl.pallas_call(
        lambda *refs: keep_kernel(own, *refs),
        out_shape=shape(3, slots, 8),
        in_specs=[VMEM],
        out_specs=VMEM,
        compiler_params=params(),
        name="keep",
    )(all_state)
    state, peak = pl.pallas_call(
        lambda *refs: change_kernel(1.0 / draws, own, *refs),
        out_shape=(state_shape, shape(mkt_count, 128)),
        in_specs=[VMEM] * 3,
        out_specs=(VMEM,) * 2,
        compiler_params=params(),
        name="change",
    )(sums, all_state, kept)
    peaks = peaks_of(peak, "mkt")
    raised, state, peak = pl.pallas_call(
        second_kernel,
        out_shape=(shape(own, slots, draws), state_shape, shape(every, 128)),
        in_specs=[VMEM] * 8,
        out_specs=(VMEM,) * 3,
        scratch_shapes=[columns, columns, *eight],
        compiler_params=params(),
        name="second",
    )(peaks, state, left, nu_near, partner, *received)
    state, rows = pl.pallas_call(
        third_kernel,
        out_shape=(state_shape, shape(draw_count, 16, 128)),
        in_specs=[VMEM] * 3,
        out_specs=(VMEM,) * 2,
        scratch_shapes=[columns, columns, *eight],
        compiler_params=params(),
        name="third",
    )(peaks_of(peak, EVERY), state, raised)
    rows = lax.all_to_all(rows, "draw", 0, 0, tiled=True)
    peak = pl.pallas_call(
        join_kernel,
        out_shape=shape(mkt_count, 128),
        in_specs=[VMEM],
        out_specs=VMEM,
        compiler_params=params(),
        name="join",
    )(rows)
    jacobian, mean_util, norms = pl.pallas_call(
        final_kernel,
        out_shape=(shape(own, slots, slots), shape(markets, slots), shape(3)),
        in_specs=[VMEM] * 4,
        out_specs=(VMEM, VMEM, SMEM),
        scratch_shapes=[pltpu.VMEM((128, draws), bf16)] * 2 + [columns, pltpu.VMEM((own, 128, 64), f32), *eight],
        compiler_params=params(),
        name="final",
    )(peaks_of(peak, "mkt"), state, rows, raised)
    return (mean_util, jacobian, norms)


def solution(mesh):
    return jax.shard_map(
        contract,
        mesh=mesh,
        in_specs=(P("mkt", None, None), P("mkt", None, "draw"), P(), P("mkt", None), P("mkt")),
        out_specs=(P("mkt", None), P(("mkt", "draw"), None, None), P()),
        check_vma=False,
    )
```
